32 devices in a mesh: strip: 32 (over z, y, x, core).
Axes of the slice: x: 2, y: 2, z: 4, core: 2. Of those that a mesh axis runs over, the one named last changes fastest.
Arguments:
- state: float32 [4096, 4096], P('strip'), may hold values from -6 to 6
- noise: float32 [4096, 4096], P('strip'), may hold values from -6 to 6
- step: float32 [1], replicated, may hold values from 0.3 to 0.7
- field_scale: float32 [1], replicated, may hold values from 0.6 to 1.2
- wave_scale: float32 [1], replicated, may hold values from 4 to 8
- source: float32 [2048, 2048], P('strip'), may hold values from -6 to 6
- obs_cells: int32 [2048], replicated, may hold values from 0 to 4194303
- obs_values: float32 [2048], replicated, may hold values from -3 to 3
Outputs:
- log_perm: float32 [2048, 2048], P('strip')
- pressure: float32 [2048, 2048], P('strip')
- loglik: float32 [], replicated
The draws below stay inside these ranges and needn't reach their ends.
Inputs may be any that keep to these rules, and one draw needn't show every extreme that they name: `obs_cells`: each entry is row * 2048 + column of an observed cell of the field grid.
All inputs are finite; a program needn't handle non-finite values.
Results may differ from the reference program's by a relative error of at most 0.00011.
Values sent between devices are 32-bit elements; how exact they have to be, the bound alone decides.
No kernel may reach another device: no remote copies, remote signals or barrier semaphores. Data moves between devices by JAX's collectives and lax.ppermute only.
A program may use at most 64 MiB of HBM per device.

```python
import math
import jax
import jax.numpy as jnp

M = 4096
N = 2048
ITERS = 4
NOBS = 2048


def place_ends(values, own_key, smallest, high):
    dims = values.shape
    spot = [jax.random.randint(jax.random.fold_in(own_key, axis), (), 0, dims[axis]) for axis in range(len(dims))]
    values = values.at[tuple(spot)].set(smallest)
    longest = dims.index(max(dims))
    spot[longest] = (spot[longest] + 1) % dims[longest]
    return values.at[tuple(spot)].set(high)


def steps_of(stream_key, shape, pieces, smallest, high):
    def one(axis_at, shards_of):
        heights = jax.random.uniform(jax.random.fold_in(jax.random.fold_in(stream_key, 6), axis_at), (shards_of,), jnp.float32, smallest / len(pieces), high / len(pieces))
        return jnp.repeat(jnp.exp(heights), shape[axis_at] // shards_of).reshape((-1,) + (1,) * (len(shape) - axis_at - 1))

    gain = one(*pieces[0])
    for cut in pieces[1:]:
        gain = gain * one(*cut)
    return gain


def centred(stream_key, extent, scale, reach, cuts=(), kind=jnp.bfloat16):
    entries = jax.random.normal(stream_key, extent, jnp.float32) * scale
    if len(cuts) > 0:
        entries = steps_of(stream_key, extent, cuts, -0.22, 0.18) * entries
    return jnp.clip(entries, min=-reach, max=reach).astype(kind)


def setup_inputs(seed: int = 0) -> dict:
    key_of = jax.random.split(jax.random.key(seed), 9)
    state = centred(key_of[0], (M, M), 1.0, 6.0, ((0, 32),), jnp.float32)
    noise = centred(key_of[1], (M, M), 1.0, 6.0, ((0, 32),), jnp.float32)
    step = jnp.clip(jax.random.uniform(key_of[2], (1,), jnp.float32, 0.3, 0.7), 0.3, 0.7)
    field_scale = jnp.clip(jax.random.uniform(key_of[3], (1,), jnp.float32, 0.6, 1.2), 0.6, 1.2)
    wave_scale = jnp.clip(jax.random.uniform(key_of[4], (1,), jnp.float32, 4.0, 8.0), 4.0, 8.0)
    source = centred(key_of[5], (N, N), 1.0, 6.0, ((0, 32),), jnp.float32)
    obs_cells = place_ends(jax.random.randint(key_of[6], (NOBS,), 0, N * N), jax.random.fold_in(key_of[6], 1), 0, (N * N) - 1).astype(jnp.int32)
    obs_values = centred(key_of[7], (NOBS,), 0.5, 3.0, (), jnp.float32)
    return {"state": state, "noise": noise, "step": step, "field_scale": field_scale, "wave_scale": wave_scale, "source": source, "obs_cells": obs_cells, "obs_values": obs_values}


def amplitude(row_freq, col_freq, length, scale, wave):
    row_wave = jnp.minimum(row_freq, length - row_freq).astype(jnp.float32)
    col_wave = jnp.minimum(col_freq, length - col_freq).astype(jnp.float32)
    shape_term = 1.0 / (1.0 + (row_wave * row_wave + col_wave * col_wave) / (wave * wave))
    return scale * length / (wave * math.sqrt(math.pi)) * shape_term

def reference(state, noise, step, field_scale, wave_scale, source, obs_cells, obs_values):
    rate = step[0]
    mixed = jnp.sqrt(1.0 - rate * rate) * state + rate * noise
    row_freq = jnp.arange(M, dtype=jnp.int32)[:, None]
    col_freq = jnp.arange(M, dtype=jnp.int32)[None, :]
    scaled = amplitude(row_freq, col_freq, M, field_scale[0], wave_scale[0])
    spectrum = jnp.fft.fft2(mixed) * scaled
    log_perm = jnp.real(jnp.fft.ifft2(spectrum))[:N, :N]
    kappa = jnp.exp(log_perm)
    padded = jnp.pad(kappa, 1)
    north = 0.5 * (kappa + padded[:-2, 1:-1])
    south = 0.5 * (kappa + padded[2:, 1:-1])
    west = 0.5 * (kappa + padded[1:-1, :-2])
    east = 0.5 * (kappa + padded[1:-1, 2:])
    diagonal = north + south + west + east

    def operate(field):
        beside_all = jnp.pad(field, 1)
        return diagonal * field - north * beside_all[:-2, 1:-1] - south * beside_all[2:, 1:-1] - west * beside_all[1:-1, :-2] - east * beside_all[1:-1, 2:]
    pressure = jnp.zeros_like(source)
    residual = source
    precond = residual / diagonal
    direction = precond
    gamma = jnp.sum(residual * precond)
    for iteration in range(ITERS):
        image = operate(direction)
        alpha = gamma / jnp.sum(direction * image)
        pressure = pressure + alpha * direction
        residual = residual - alpha * image
        if iteration + 1 < ITERS:
            precond = residual / diagonal
            fresh = jnp.sum(residual * precond)
            direction = precond + fresh / gamma * direction
            gamma = fresh
    picked = pressure.reshape(-1)[obs_cells]
    differ = picked - obs_values
    loglik = -(2.0 / NOBS) * jnp.sum(differ * differ)
    return (log_perm, pressure, loglik)
```

```python
import functools
import math

import jax
import jax.numpy as jnp
import numpy as np
from jax import lax
from jax.experimental import pallas as pl
from jax.experimental.pallas import tpu as pltpu
from jax.sharding import PartitionSpec as P

ITERS = 4
LANES = 128
HALO = 8
TERMS = 2 * ITERS
PAIRS = [(i, j) for i in range(ITERS) for j in range(i, ITERS)]
SUMS = TERMS + len(PAIRS) + ITERS


def mm(left, right):
    return lax.dot_general(
        left,
        right,
        (((1,), (0,)), ((), ())),
        precision=lax.Precision.HIGHEST,
        preferred_element_type=jnp.float32,
    )


def dft_tables():
    spot = np.arange(LANES)
    angle = 2.0 * np.pi * np.outer(spot, spot) / LANES
    cos, sin = np.cos(angle), np.sin(angle)
    forward = np.block([[cos, -sin], [sin, cos]])
    inverse = np.block([[cos, sin], [-sin, cos]])
    half = LANES // 2
    whole = 2.0 * np.pi * np.outer(spot, np.arange(1, half)) / LANES
    edge = np.ones((LANES, 1))
    alternate = ((-1.0) ** spot)[:, None]
    zero_f = np.concatenate([edge, np.cos(whole), alternate, -np.sin(whole)], 1)
    zero_i = np.concatenate([edge, 2 * np.cos(whole), alternate, -2 * np.sin(whole)], 1).T
    odd = 2.0 * np.pi * np.outer(spot, np.arange(half) + 0.5) / LANES
    half_f = np.concatenate([np.cos(odd), -np.sin(odd)], 1)
    half_i = 2.0 * np.concatenate([np.cos(odd), -np.sin(odd)], 1).T
    none = np.zeros((LANES, LANES))
    special_f = np.block([[zero_f, none], [none, half_f]])
    special_i = np.block([[zero_i, none], [none, half_i]])
    return forward, inverse, special_f, special_i


def twiddle_table(length, factor):
    angle = 2.0 * np.pi * np.outer(np.arange(factor // 2), np.arange(LANES)) / length
    return np.cos(angle), np.sin(angle)


def times(value, factor):
    if value is None or factor == 0.0:
        return None
    if factor == 1.0:
        return value
    if factor == -1.0:
        return -value
    return value * factor


def plus(left, right):
    if left is None:
        return right
    if right is None:
        return left
    return left + right


def minus(left, right):
    if right is None:
        return left
    if left is None:
        return -right
    return left - right


def root(k, n):
    quarter = (8 * k) % (8 * n)
    if quarter % n == 0 and (quarter // n) % 2 == 0:
        return ((1.0, 0.0), (0.0, 1.0), (-1.0, 0.0), (0.0, -1.0))[(quarter // n) // 2]
    return (math.cos(2 * math.pi * k / n), math.sin(2 * math.pi * k / n))


def rotate(re, im, c, s):
    return (
        minus(times(re, c), times(im, s)),
        plus(times(re, s), times(im, c)),
    )


def rfft(values):
    n = len(values)
    if n == 2:
        return [(values[0] + values[1], None), (values[0] - values[1], None)]
    even = rfft(values[0::2])
    odd = rfft(values[1::2])
    out = [None] * (n // 2 + 1)
    for k in range(n // 4 + 1):
        c, s = root(k, n)
        tr, ti = rotate(odd[k][0], odd[k][1], c, -s)
        er, ei = even[k]
        out[k] = (plus(er, tr), plus(ei, ti))
        if k != n // 4:
            out[n // 2 - k] = (minus(er, tr), minus(ti, ei))
    return out


def irfft(spectrum, n):
    if n == 2:
        return [spectrum[0][0] + spectrum[1][0]]
    even, odd = [], []
    for k in range(n // 4 + 1):
        ar, ai = spectrum[k]
        br, bi = spectrum[n // 2 - k]
        if k == n // 4:
            even.append((2.0 * ar, None))
            odd.append((-2.0 * ai, None))
            continue
        even.append((plus(ar, br), minus(ai, bi)))
        c, s = root(k, n)
        odd.append(rotate(minus(ar, br), plus(ai, bi), c, s))
    even = irfft(even, n // 2)
    odd = irfft(odd, n // 2)
    return [value for pair in zip(even, odd) for value in pair]


def row_kernel(step, state, noise, twiddle, pair_w, special_w, out, work, *, factor):
    rows = state.shape[0]
    half = factor // 2
    rate = step[0]
    keep = jnp.sqrt(jnp.full((8, LANES), 1.0 - rate * rate, jnp.float32))

    def group(index, carry):
        base = pl.multiple_of(index * 8, 8)
        tiles = [
            keep * state[pl.ds(base, 8), LANES * a : LANES * (a + 1)]
            + rate * noise[pl.ds(base, 8), LANES * a : LANES * (a + 1)]
            for a in range(factor)
        ]
        spectrum = rfft(tiles)
        work[0, pl.ds(base, 8), :LANES] = spectrum[0][0]
        work[0, pl.ds(base, 8), LANES:] = spectrum[half][0]
        for j in range(1, half):
            c = twiddle[j : j + 1, :]
            s = twiddle[half + j : half + j + 1, :]
            re, im = spectrum[j]
            work[j, pl.ds(base, 8), :LANES] = re * c + im * s
            work[j, pl.ds(base, 8), LANES:] = im * c - re * s
        return carry

    lax.fori_loop(0, rows // 8, group, 0)
    first = mm(work[0], special_w[...])
    out[0] = first[:, :LANES]
    out[1] = first[:, LANES:]
    for j in range(1, half):
        value = mm(work[j], pair_w[...])
        out[2 * j] = value[:, :LANES]
        out[2 * j + 1] = value[:, LANES:]


def row_forward(state, noise, step, tables):
    rows, length = state.shape
    factor = length // LANES
    block = min(32, rows)
    twiddle, pair_w, special_w = tables
    whole = lambda i: (0, 0)
    return pl.pallas_call(
        functools.partial(row_kernel, factor=factor),
        grid=(rows // block,),
        in_specs=[
            pl.BlockSpec(memory_space=pltpu.SMEM),
            pl.BlockSpec((block, length), lambda i: (i, 0)),
            pl.BlockSpec((block, length), lambda i: (i, 0)),
            pl.BlockSpec(twiddle.shape, whole),
            pl.BlockSpec(pair_w.shape, whole),
            pl.BlockSpec(special_w.shape, whole),
        ],
        out_specs=pl.BlockSpec((factor, block, LANES), lambda i: (0, i, 0)),
        out_shape=jax.ShapeDtypeStruct((factor, rows, LANES), jnp.float32),
        scratch_shapes=[pltpu.VMEM((factor // 2, block, 2 * LANES), jnp.float32)],
        name="row_forward",
    )(step, state, noise, twiddle, pair_w, special_w)


def column_kernel(
    scale, column, table, forward_w, special_f, inverse_w, special_i, wave, out, work, field, *, field_rows
):
    factor, _, width = column.shape
    half = factor // 2
    length = factor * LANES
    parts = out.shape[0]

    def ahead(index, carry):
        base = pl.multiple_of(index * 8, 8)
        spectrum = rfft([column[a, pl.ds(base, 8), :] for a in range(factor)])
        low = pl.ds(base, 8)
        high = pl.ds(pl.multiple_of(base + LANES, 8), 8)
        work[0, low, :] = spectrum[0][0]
        work[0, high, :] = spectrum[half][0]
        turn = table[low, :]
        for j in range(1, half):
            c = turn[:, j : j + 1]
            s = turn[:, half + j : half + j + 1]
            re, im = spectrum[j]
            work[j, low, :] = re * c + im * s
            work[j, high, :] = im * c - re * s
        return carry

    lax.fori_loop(0, LANES // 8, ahead, 0)
    place = lax.broadcasted_iota(jnp.int32, (LANES, width), 0)
    side = wave[...] + scale[1]
    gain = scale[0]

    def amplitude(freq):
        freq = jnp.minimum(freq, length - freq).astype(jnp.float32)
        return gain / (freq * freq + side)

    for j in range(half):
        if j == 0:
            value = mm(special_f[...], work[0])
            halves = LANES // 2
            top = amplitude(factor * jnp.where(place > halves, place - halves, place))
            low = amplitude(half + factor * jnp.where(place >= halves, place - halves, place))
            value = jnp.concatenate([value[:LANES] * top, value[LANES:] * low], axis=0)
            work[0] = mm(special_i[...], value)
        else:
            value = mm(forward_w[...], work[j])
            top = amplitude(j + factor * place)
            value = jnp.concatenate([value[:LANES] * top, value[LANES:] * top], axis=0)
            work[j] = mm(inverse_w[...], value)

    rim = jnp.zeros((HALO, width), jnp.float32)
    field[:HALO, :] = rim
    field[HALO + length // 2 :, :] = rim

    def back(index, carry):
        base = pl.multiple_of(index * 8, 8)
        low = pl.ds(base, 8)
        high = pl.ds(pl.multiple_of(base + LANES, 8), 8)
        turn = table[low, :]
        spectrum = [(work[0, low, :], None)]
        for j in range(1, half):
            c = turn[:, j : j + 1]
            s = turn[:, half + j : half + j + 1]
            re, im = work[j, low, :], work[j, high, :]
            spectrum.append((re * c - im * s, re * s + im * c))
        spectrum.append((work[0, high, :], None))
        values = irfft(spectrum, factor)
        for a in range(half):
            field[pl.ds(pl.multiple_of(base + HALO + LANES * a, 8), 8), :] = values[a]
        return carry

    lax.fori_loop(0, LANES // 8, back, 0)
    for part in range(parts):
        out[part] = field[field_rows * part : field_rows * (part + 1) + 2 * HALO, :]


def column_filter(column, scale, wave, tables, parts, field_rows):
    factor, _, width = column.shape
    length = factor * LANES
    vmem = pl.BlockSpec(memory_space=pltpu.VMEM)
    return pl.pallas_call(
        functools.partial(column_kernel, field_rows=field_rows),
        in_specs=[pl.BlockSpec(memory_space=pltpu.SMEM)] + [vmem] * 7,
        out_specs=vmem,
        out_shape=jax.ShapeDtypeStruct((parts, field_rows + 2 * HALO, width), jnp.float32),
        scratch_shapes=[
            pltpu.VMEM((factor // 2, 2 * LANES, width), jnp.float32),
            pltpu.VMEM((length // 2 + 2 * HALO, width), jnp.float32),
        ],
        name="column_filter",
    )(scale, column, *tables, wave)


def observe_kernel(local, cells, values, count, total, left):
    rows, columns = count.shape
    block = columns
    origin = pl.program_id(0) * block

    @pl.when(pl.program_id(0) == 0)
    def _():
        row = lax.broadcasted_iota(jnp.int32, (rows, local.shape[1]), 0)
        here = row == local[...]
        value = jnp.broadcast_to(values[...], here.shape)
        first = value.astype(jnp.bfloat16).astype(jnp.float32)
        second = (value - first).astype(jnp.bfloat16).astype(jnp.float32)
        third = value - first - second
        for slot, piece in enumerate((1.0, first, second, third)):
            left[slot * rows : (slot + 1) * rows, :] = jnp.where(here, piece, 0.0).astype(jnp.bfloat16)

    spot = lax.broadcasted_iota(jnp.int32, (block, local.shape[1]), 0) + origin
    right = jnp.where(spot == cells[...], 1.0, 0.0).astype(jnp.bfloat16)
    result = lax.dot_general(
        left[...], right, (((1,), (1,)), ((), ())), preferred_element_type=jnp.float32
    )
    count[...] = result[:rows]
    total[...] = (result[3 * rows :] + result[2 * rows : 3 * rows]) + result[rows : 2 * rows]


def observe(local_row, cell_col, values, rows, columns):
    number = values.shape[1]
    block = 256
    whole = pl.BlockSpec((1, number), lambda i: (0, 0))
    piece = pl.BlockSpec((rows, block), lambda i: (0, i))
    shape = jax.ShapeDtypeStruct((rows, columns), jnp.float32)
    return pl.pallas_call(
        observe_kernel,
        grid=(columns // block,),
        in_specs=[whole, whole, whole],
        out_specs=(piece, piece),
        out_shape=(shape, shape),
        scratch_shapes=[pltpu.VMEM((4 * rows, number), jnp.bfloat16)],
        cost_estimate=pl.CostEstimate(
            flops=8 * rows * number * columns, transcendentals=0, bytes_accessed=8 * rows * columns
        ),
        name="observe",
    )(local_row, cell_col, values)


def two_sum(a, b):
    s = a + b
    t = s - a
    return s, (a - (s - t)) + (b - t)


def split(a):
    t = a * 4097.0
    high = t - (t - a)
    return high, a - high


def two_prod(a, b):
    p = a * b
    ah, al = split(a)
    bh, bl = split(b)
    return p, ((ah * bh - p) + ah * bl + al * bh) + al * bl


def dd_add(x, y):
    s, e = two_sum(x[0], y[0])
    e = e + (x[1] + y[1])
    high = s + e
    return high, e - (high - s)


def dd_neg(x):
    return -x[0], -x[1]


def dd_mul(x, y):
    p, e = two_prod(x[0], y[0])
    e = e + (x[0] * y[1] + x[1] * y[0])
    high = p + e
    return high, e - (high - p)


def dd_div(x, y):
    first = x[0] / y[0]
    rest = dd_add(x, dd_neg(dd_mul(y, (first, jnp.zeros_like(first)))))
    second = rest[0] / y[0]
    rest = dd_add(rest, dd_neg(dd_mul(y, (second, jnp.zeros_like(first)))))
    third = rest[0] / y[0]
    high, low = two_sum(first, second)
    return dd_add((high, low), (third, jnp.zeros_like(third)))


def fold(high, low, shift, axis):
    other, error = two_sum(high, pltpu.roll(high, shift, axis))
    return other, (low + pltpu.roll(low, shift, axis)) + error


def tile_sum(value):
    pieces = [value[:, LANES * i : LANES * (i + 1)] for i in range(value.shape[1] // LANES)]
    while len(pieces) > 1:
        pieces = [a + b for a, b in zip(pieces[0::2], pieces[1::2])]
    return pieces[0]


def krylov_kernel(
    origin, coefs, source, count, total, twiddle, inverse_w, special_i,
    log_perm, basis, partial,
    work, kappa, centre, inverse, north, south, west, east, vector,
):
    factor, extent, _ = coefs.shape
    half = factor // 2
    columns = half * LANES
    rows = extent - 2 * HALO
    groups = extent // 8
    pair = jnp.concatenate([coefs[0], coefs[1]], axis=1)
    work[0] = mm(pair, special_i[...])
    for j in range(1, half):
        pair = jnp.concatenate([coefs[2 * j], coefs[2 * j + 1]], axis=1)
        work[j] = mm(pair, inverse_w[...])

    rim = jnp.zeros((8, columns), jnp.float32)
    for ref in (kappa, vector.at[0], vector.at[1]):
        ref[:8, :] = rim
        ref[8 + extent :, :] = rim

    first_row = origin[0] - HALO
    limit = origin[1]

    def inverse_group(index, carry):
        base = pl.multiple_of(index * 8, 8)
        low = pl.ds(base, 8)
        spectrum = [(work[0, low, :LANES], None)]
        for j in range(1, half):
            c = twiddle[j : j + 1, :]
            s = twiddle[half + j : half + j + 1, :]
            re, im = work[j, low, :LANES], work[j, low, LANES:]
            spectrum.append((re * c - im * s, re * s + im * c))
        spectrum.append((work[0, low, LANES:], None))
        values = irfft(spectrum, factor)
        row = lax.broadcasted_iota(jnp.int32, (8, LANES), 0) + (base + first_row)
        valid = (row >= 0) & (row < limit)
        store = pl.ds(pl.multiple_of(base + 8, 8), 8)
        for a in range(half):
            kappa[store, LANES * a : LANES * (a + 1)] = jnp.where(valid, jnp.exp(values[a]), 0.0)

        @pl.when((index >= HALO // 8) & (index < groups - HALO // 8))
        def _():
            own = pl.ds(pl.multiple_of(base - HALO, 8), 8)
            for a in range(half):
                log_perm[own, LANES * a : LANES * (a + 1)] = values[a]

        return carry

    lax.fori_loop(0, groups, inverse_group, 0)

    lane = lax.broadcasted_iota(jnp.int32, (8, columns), 1)
    inner_west = lane > 0
    inner_east = lane < columns - 1
    zero = jnp.zeros((8, LANES), jnp.float32)
    sums = [zero] * SUMS

    for group in range(groups):
        at = 8 + 8 * group
        own = HALO // 8 <= group < groups - HALO // 8
        here = kappa[at : at + 8, :]
        up = 0.5 * (here + kappa[at - 1 : at + 7, :])
        down = 0.5 * (here + kappa[at + 1 : at + 9, :])
        left = jnp.where(inner_west, pltpu.roll(here, 1, 1), 0.0)
        right = jnp.where(inner_east, pltpu.roll(here, columns - 1, 1), 0.0)
        left = 0.5 * (here + left)
        right = 0.5 * (here + right)
        middle = up + down + left + right
        row = lax.broadcasted_iota(jnp.int32, (8, columns), 0) + (8 * group + first_row)
        rest = jnp.where((row >= 0) & (row < limit), 1.0 / middle, 0.0)
        put = slice(8 * group, 8 * group + 8)
        centre[put, :] = middle
        inverse[put, :] = rest
        north[put, :] = up
        south[put, :] = down
        west[put, :] = jnp.where(inner_west, left, 0.0)
        east[put, :] = jnp.where(inner_east, right, 0.0)
        first = source[put, :]
        value = first * rest
        vector[0, at : at + 8, :] = value
        if own:
            basis[0, 8 * group - HALO : 8 * group - HALO + 8, :] = value
            sums[0] = sums[0] + tile_sum(first * value)

    for step in range(ITERS):
        now = vector.at[step % 2]
        new = vector.at[(step + 1) % 2]
        for group in range(groups):
            at = 8 + 8 * group
            own = HALO // 8 <= group < groups - HALO // 8
            if step == ITERS - 1 and not own:
                continue
            put = slice(8 * group, 8 * group + 8)
            here = now[at : at + 8, :]
            image = (
                centre[put, :] * here
                - north[put, :] * now[at - 1 : at + 7, :]
                - south[put, :] * now[at + 1 : at + 9, :]
                - west[put, :] * pltpu.roll(here, 1, 1)
                - east[put, :] * pltpu.roll(here, columns - 1, 1)
            )
            if own:
                sums[2 * step + 1] = sums[2 * step + 1] + tile_sum(here * image)
            if step < ITERS - 1:
                value = image * inverse[put, :]
                new[at : at + 8, :] = value
                if own:
                    basis[step + 1, 8 * group - HALO : 8 * group - HALO + 8, :] = value
                    sums[2 * step + 2] = sums[2 * step + 2] + tile_sum(value * image)

    for group in range(rows // 8):
        put = slice(8 * group, 8 * group + 8)
        vectors = [basis[k, put, :] for k in range(ITERS)]
        weight = count[put, :]
        weighted = [weight * v for v in vectors]
        for spot, (i, j) in enumerate(PAIRS):
            sums[TERMS + spot] = sums[TERMS + spot] + tile_sum(weighted[i] * vectors[j])
        datum = total[put, :]
        for k in range(ITERS):
            slot = TERMS + len(PAIRS) + k
            sums[slot] = sums[slot] + tile_sum(datum * vectors[k])

    sub = lax.broadcasted_iota(jnp.int32, (8, LANES), 0)
    spot = lax.broadcasted_iota(jnp.int32, (8, LANES), 1)
    row = zero
    for begin in range(0, SUMS, 8):
        high, low = zero, zero
        for k in range(begin, min(begin + 8, SUMS)):
            h, e = sums[k], zero
            for shift in (4, 2, 1):
                h, e = fold(h, e, shift, 0)
            high = jnp.where(sub == k - begin, h, high)
            low = jnp.where(sub == k - begin, e, low)
        for shift in (64, 32, 16, 8, 4, 2, 1):
            high, low = fold(high, low, shift, 1)
        row = row + jnp.where(spot == sub + begin, high, 0.0)
        row = row + jnp.where(spot == sub + begin + LANES // 2, low, 0.0)
    for shift in (4, 2, 1):
        row = row + pltpu.roll(row, shift, 0)
    for part in range(partial.shape[0]):
        partial[part] = row[:1]


def krylov(origin, coefs, source, count, total, tables, parts):
    factor, extent, _ = coefs.shape
    columns = factor // 2 * LANES
    rows = extent - 2 * HALO
    vmem = pl.BlockSpec(memory_space=pltpu.VMEM)
    plane = pltpu.VMEM((extent, columns), jnp.float32)
    padded = pltpu.VMEM((extent + 16, columns), jnp.float32)
    return pl.pallas_call(
        krylov_kernel,
        in_specs=[pl.BlockSpec(memory_space=pltpu.SMEM)] + [vmem] * 7,
        out_specs=(vmem, vmem, vmem),
        out_shape=(
            jax.ShapeDtypeStruct((rows, columns), jnp.float32),
            jax.ShapeDtypeStruct((ITERS, rows, columns), jnp.float32),
            jax.ShapeDtypeStruct((parts, 1, LANES), jnp.float32),
        ),
        scratch_shapes=[
            pltpu.VMEM((factor // 2, extent, 2 * LANES), jnp.float32),
            padded,
            plane,
            plane,
            plane,
            plane,
            plane,
            plane,
            pltpu.VMEM((2, extent + 16, columns), jnp.float32),
        ],
        name="krylov",
    )(origin, coefs, source, count, total, *tables)


def final_kernel(partial, basis, values, pressure, loglik):
    parts = partial.shape[0]
    high = jnp.concatenate([partial[k] for k in range(parts)], axis=0)
    low = pltpu.roll(high, LANES // 2, 1)
    while high.shape[0] > 8:
        middle = high.shape[0] // 2
        top, error = two_sum(high[:middle], high[middle:])
        low = (low[:middle] + low[middle:]) + error
        high = top
    for shift in (4, 2, 1):
        high, low = fold(high, low, shift, 0)

    def pick(k):
        return (
            jnp.broadcast_to(high[:, k : k + 1], (8, LANES)),
            jnp.broadcast_to(low[:, k : k + 1], (8, LANES)),
        )

    moments = [pick(k) for k in range(TERMS)]
    matrix = [[moments[i + j + 1] for j in range(ITERS)] for i in range(ITERS)]
    right = [moments[i] for i in range(ITERS)]
    for i in range(ITERS):
        for r in range(i + 1, ITERS):
            ratio = dd_neg(dd_div(matrix[i][r], matrix[i][i]))
            for c in range(r, ITERS):
                matrix[r][c] = dd_add(matrix[r][c], dd_mul(ratio, matrix[i][c]))
            right[r] = dd_add(right[r], dd_mul(ratio, right[i]))
    weights = [None] * ITERS
    for i in reversed(range(ITERS)):
        value = right[i]
        for c in range(i + 1, ITERS):
            value = dd_add(value, dd_neg(dd_mul(matrix[i][c], weights[c])))
        weights[i] = dd_div(value, matrix[i][i])

    data = values[...]
    h, e = two_prod(data, data)
    while h.shape[0] > 8:
        middle = h.shape[0] // 2
        top, error = two_sum(h[:middle], h[middle:])
        e = (e[:middle] + e[middle:]) + error
        h = top
    for shift in (4, 2, 1):
        h, e = fold(h, e, shift, 0)
    for shift in (64, 32, 16, 8, 4, 2, 1):
        h, e = fold(h, e, shift, 1)
    misfit = (h, e)
    for spot, (i, j) in enumerate(PAIRS):
        term = dd_mul(dd_mul(weights[i], weights[j]), pick(TERMS + spot))
        misfit = dd_add(misfit, term)
        if i != j:
            misfit = dd_add(misfit, term)
    for k in range(ITERS):
        term = dd_neg(dd_mul(weights[k], pick(TERMS + len(PAIRS) + k)))
        misfit = dd_add(misfit, dd_add(term, term))
    number = values.shape[0] * LANES
    loglik[...] = (-(2.0 / number) * (misfit[0] + misfit[1]))[:1, :]

    factors = [w[0][:1, :1] for w in weights]
    for group in range(pressure.shape[0] // 8):
        put = slice(8 * group, 8 * group + 8)
        value = factors[0] * basis[0, put, :]
        for k in range(1, ITERS):
            value = value + factors[k] * basis[k, put, :]
        pressure[put, :] = value


def finish(partial, basis, values):
    vmem = pl.BlockSpec(memory_space=pltpu.VMEM)
    return pl.pallas_call(
        final_kernel,
        in_specs=[vmem] * 3,
        out_specs=(vmem, vmem),
        out_shape=(
            jax.ShapeDtypeStruct(basis.shape[1:], jnp.float32),
            jax.ShapeDtypeStruct((1, LANES), jnp.float32),
        ),
        name="finish",
    )(partial, basis, values)


def exchange(block):
    return lax.all_to_all(block, "strip", split_axis=0, concat_axis=0, tiled=True)


def body(state, noise, step, field_scale, wave_scale, source, obs_cells, obs_values):
    parts = lax.axis_size("strip")
    position = lax.axis_index("strip")
    rows_here, length = state.shape
    factor = length // LANES
    half = factor // 2
    width = length // parts
    ways = parts // factor
    field_rows, columns = source.shape

    forward, inverse, special_f, special_i = (np.float32(t) for t in dft_tables())
    cos, sin = twiddle_table(length, factor)
    across = np.float32(np.concatenate([cos, sin], 0))
    down = np.zeros((LANES, LANES), np.float32)
    down[:, :factor] = across.T

    ahead = [(i, i + 1) for i in range(parts - 1)]
    behind = [(b, a) for a, b in ahead]
    above = lax.ppermute(source[field_rows - HALO :], "strip", ahead)
    below = lax.ppermute(source[:HALO], "strip", behind)
    wide_source = jnp.concatenate([above, source, below], axis=0)

    cell_row = obs_cells // columns - position * field_rows
    count, total = observe(
        cell_row[None, :], (obs_cells % columns)[None, :], obs_values[None, :], field_rows, columns
    )

    tiles = row_forward(state, noise, step, (across, forward, special_f))
    if ways > 1:
        tiles = tiles.reshape(factor, rows_here, ways, width).transpose(0, 2, 1, 3)
        tiles = tiles.reshape(parts, rows_here, width)
    column = exchange(tiles).reshape(factor, LANES, width)

    slot = position * width + lax.broadcasted_iota(jnp.int32, (1, width), 1)
    tile, lane = slot // LANES, slot % LANES
    middle = LANES // 2
    freq = jnp.where(
        tile == 0,
        factor * jnp.where(lane > middle, lane - middle, lane),
        jnp.where(
            tile == 1,
            half + factor * jnp.where(lane >= middle, lane - middle, lane),
            tile // 2 + factor * lane,
        ),
    )
    freq = jnp.minimum(freq, length - freq).astype(jnp.float32)
    wave = wave_scale[0]
    gain = field_scale[0] * wave / (math.sqrt(math.pi) * length)
    scale = jnp.stack([gain, wave * wave])
    blocks = column_filter(
        column,
        scale,
        freq * freq,
        (down, forward.T, special_f.T, inverse.T, special_i.T),
        parts,
        field_rows,
    )
    coefs = exchange(blocks)
    extent = field_rows + 2 * HALO
    if ways > 1:
        coefs = coefs.reshape(factor, ways, extent, width).transpose(0, 2, 1, 3)
        coefs = coefs.reshape(factor, extent, LANES)

    origin = jnp.stack([position * field_rows, parts * field_rows]).astype(jnp.int32)
    log_perm, basis, partial = krylov(
        origin, coefs, wide_source, count, total, (across, inverse, special_i), parts
    )
    pressure, loglik = finish(exchange(partial), basis, obs_values.reshape(-1, LANES))
    return (log_perm, pressure, loglik[0, 0])


def solution(mesh):
    placed = (P("strip", None), P("strip", None), P(), P(), P(), P("strip", None), P(), P())
    return jax.shard_map(
        body,
        mesh=mesh,
        in_specs=placed,
        out_specs=(P("strip", None), P("strip", None), P()),
        check_vma=False,
    )
```

```python
import functools
import math

import jax
import jax.numpy as jnp
import numpy as np
from jax import lax
from jax.experimental import pallas as pl
from jax.experimental.pallas import tpu as pltpu
from jax.sharding import PartitionSpec as P

ITERS = 4
LANES = 128
HALO = 8
ABOVE = ITERS
BELOW = ITERS + 1
TERMS = 2 * ITERS
PAIRS = [(i, j) for i in range(ITERS) for j in range(i, ITERS)]
SUMS = TERMS + len(PAIRS) + ITERS


def dot(left, right):
    return lax.dot_general(
        left, right, (((1,), (0,)), ((), ())), preferred_element_type=jnp.float32
    )


def halves(value):
    high = value.astype(jnp.bfloat16)
    return high, (value - high.astype(jnp.float32)).astype(jnp.bfloat16)


def rows_times(value, table):
    size = value.shape[1]
    high, low = halves(value)
    upper = table[:size, :]
    return dot(high, table[size:, :]) + dot(low, upper) + dot(high, upper)


def times_columns(table, value):
    size = value.shape[0]
    high, low = halves(value)
    upper = table[:size, :]
    return dot(table[size:, :], high) + dot(upper, low) + dot(upper, high)


def pieces(table):
    table = np.asarray(table, np.float64)
    high = table.astype(jnp.bfloat16)
    low = (table - high.astype(np.float64)).astype(jnp.bfloat16)
    return np.concatenate([high, low], 0)


def near(value):
    return pltpu.with_memory_space_constraint(value, pltpu.VMEM)


def far(value):
    return pltpu.with_memory_space_constraint(value, pltpu.HBM)


def dft_tables():
    spot = np.arange(LANES)
    angle = 2.0 * np.pi * np.outer(spot, spot) / LANES
    cos, sin = np.cos(angle), np.sin(angle)
    forward = np.block([[cos, -sin], [sin, cos]])
    inverse = np.block([[cos, sin], [-sin, cos]])
    half = LANES // 2
    whole = 2.0 * np.pi * np.outer(spot, np.arange(1, half)) / LANES
    edge = np.ones((LANES, 1))
    alternate = ((-1.0) ** spot)[:, None]
    zero_f = np.concatenate([edge, np.cos(whole), alternate, -np.sin(whole)], 1)
    zero_i = np.concatenate([edge, 2 * np.cos(whole), alternate, -2 * np.sin(whole)], 1).T
    odd = 2.0 * np.pi * np.outer(spot, np.arange(half) + 0.5) / LANES
    half_f = np.concatenate([np.cos(odd), -np.sin(odd)], 1)
    half_i = 2.0 * np.concatenate([np.cos(odd), -np.sin(odd)], 1).T
    none = np.zeros((LANES, LANES))
    special_f = np.block([[zero_f, none], [none, half_f]])
    special_i = np.block([[zero_i, none], [none, half_i]])
    return forward, inverse, special_f, special_i


def twiddle_table(length, factor):
    angle = 2.0 * np.pi * np.outer(np.arange(factor // 2), np.arange(LANES)) / length
    return np.cos(angle), np.sin(angle)


def times(value, factor):
    if value is None or factor == 0.0:
        return None
    if factor == 1.0:
        return value
    if factor == -1.0:
        return -value
    return value * factor


def plus(left, right):
    if left is None:
        return right
    if right is None:
        return left
    return left + right


def minus(left, right):
    if right is None:
        return left
    if left is None:
        return -right
    return left - right


def root(k, n):
    quarter = (8 * k) % (8 * n)
    if quarter % n == 0 and (quarter // n) % 2 == 0:
        return ((1.0, 0.0), (0.0, 1.0), (-1.0, 0.0), (0.0, -1.0))[(quarter // n) // 2]
    return (math.cos(2 * math.pi * k / n), math.sin(2 * math.pi * k / n))


def rotate(re, im, c, s):
    return (
        minus(times(re, c), times(im, s)),
        plus(times(re, s), times(im, c)),
    )


def rfft(values):
    n = len(values)
    if n == 2:
        return [(values[0] + values[1], None), (values[0] - values[1], None)]
    even = rfft(values[0::2])
    odd = rfft(values[1::2])
    out = [None] * (n // 2 + 1)
    for k in range(n // 4 + 1):
        c, s = root(k, n)
        tr, ti = rotate(odd[k][0], odd[k][1], c, -s)
        er, ei = even[k]
        out[k] = (plus(er, tr), plus(ei, ti))
        if k != n // 4:
            out[n // 2 - k] = (minus(er, tr), minus(ti, ei))
    return out


def irfft(spectrum, n):
    if n == 2:
        return [spectrum[0][0] + spectrum[1][0]]
    even, odd = [], []
    for k in range(n // 4 + 1):
        ar, ai = spectrum[k]
        br, bi = spectrum[n // 2 - k]
        if k == n // 4:
            even.append((2.0 * ar, None))
            odd.append((-2.0 * ai, None))
            continue
        even.append((plus(ar, br), minus(ai, bi)))
        c, s = root(k, n)
        odd.append(rotate(minus(ar, br), plus(ai, bi), c, s))
    even = irfft(even, n // 2)
    odd = irfft(odd, n // 2)
    return [value for pair in zip(even, odd) for value in pair]


def row_kernel(step, state, noise, twiddle, pair_w, special_w, out, work, *, factor):
    rows = state.shape[0]
    half = factor // 2
    rate = step[0]
    keep = jnp.sqrt(jnp.full((8, LANES), 1.0 - rate * rate, jnp.float32))

    def group(index, carry):
        base = pl.multiple_of(index * 8, 8)
        tiles = [
            keep * state[pl.ds(base, 8), LANES * a : LANES * (a + 1)]
            + rate * noise[pl.ds(base, 8), LANES * a : LANES * (a + 1)]
            for a in range(factor)
        ]
        spectrum = rfft(tiles)
        work[0, pl.ds(base, 8), :LANES] = spectrum[0][0]
        work[0, pl.ds(base, 8), LANES:] = spectrum[half][0]
        for j in range(1, half):
            c = twiddle[j : j + 1, :]
            s = twiddle[half + j : half + j + 1, :]
            re, im = spectrum[j]
            work[j, pl.ds(base, 8), :LANES] = re * c + im * s
            work[j, pl.ds(base, 8), LANES:] = im * c - re * s
        return carry

    lax.fori_loop(0, rows // 8, group, 0, unroll=4)
    put = slice(None)
    first = rows_times(work[0], special_w)
    out[0, put, :] = first[:, :LANES]
    out[1, put, :] = first[:, LANES:]
    batch = 5
    for begin in range(1, half, batch):
        value = rows_times(work[begin : begin + batch].reshape(batch * rows, 2 * LANES), pair_w)
        for k in range(batch):
            out[2 * (begin + k), put, :] = value[k * rows : (k + 1) * rows, :LANES]
            out[2 * (begin + k) + 1, put, :] = value[k * rows : (k + 1) * rows, LANES:]


def row_forward(state, noise, step, tables):
    rows, length = state.shape
    factor = length // LANES
    block = min(32, rows)
    twiddle, pair_w, special_w = tables
    whole = lambda i: (0, 0)
    return pl.pallas_call(
        functools.partial(row_kernel, factor=factor),
        grid=(rows // block,),
        in_specs=[
            pl.BlockSpec(memory_space=pltpu.SMEM),
            pl.BlockSpec((block, length), lambda i: (i, 0)),
            pl.BlockSpec((block, length), lambda i: (i, 0)),
            pl.BlockSpec(twiddle.shape, whole),
            pl.BlockSpec(pair_w.shape, whole),
            pl.BlockSpec(special_w.shape, whole),
        ],
        out_specs=pl.BlockSpec((factor, block, LANES), lambda i: (0, i, 0)),
        out_shape=pltpu.HBM((factor, rows, LANES), jnp.float32),
        scratch_shapes=[pltpu.VMEM((factor // 2, block, 2 * LANES), jnp.float32)],
        compiler_params=pltpu.CompilerParams(vmem_limit_bytes=16 << 20),
        name="row_forward",
    )(step, far(state), far(noise), far(twiddle), far(pair_w), far(special_w))


def column_kernel(
    scale, column, table, forward_w, special_f, inverse_w, special_i, wave, out, work, field, *, field_rows
):
    factor, _, width = column.shape
    half = factor // 2
    length = factor * LANES
    extent = field_rows + ABOVE + BELOW

    def ahead(index, carry):
        base = pl.multiple_of(index * 8, 8)
        spectrum = rfft([column[a, pl.ds(base, 8), :] for a in range(factor)])
        low = pl.ds(base, 8)
        high = pl.ds(pl.multiple_of(base + LANES, 8), 8)
        work[0, low, :] = spectrum[0][0]
        work[0, high, :] = spectrum[half][0]
        turn = table[low, :]
        for j in range(1, half):
            c = turn[:, j : j + 1]
            s = turn[:, half + j : half + j + 1]
            re, im = spectrum[j]
            work[j, low, :] = re * c + im * s
            work[j, high, :] = im * c - re * s
        return carry

    lax.fori_loop(0, LANES // 8, ahead, 0, unroll=4)
    place = lax.broadcasted_iota(jnp.int32, (LANES, width), 0)
    side = wave[...] + scale[1]
    gain = scale[0]

    def amplitude(freq):
        freq = jnp.minimum(freq, length - freq).astype(jnp.float32)
        return gain / (freq * freq + side)

    batch = 2 if width % LANES == 0 else 1
    for j in range(half):
        if j == 0:
            value = times_columns(special_f, work[0])
            middle = LANES // 2
            top = amplitude(factor * jnp.where(place > middle, place - middle, place))
            low = amplitude(half + factor * jnp.where(place >= middle, place - middle, place))
            value = jnp.concatenate([value[:LANES] * top, value[LANES:] * low], axis=0)
            work[0] = times_columns(special_i, value)
            continue
        if (j - 1) % batch:
            continue
        block = range(j, min(j + batch, half))
        value = times_columns(forward_w, jnp.concatenate([work[k] for k in block], axis=1))
        top = jnp.concatenate([amplitude(k + factor * place) for k in block], axis=1)
        value = jnp.concatenate([value[:LANES] * top, value[LANES:] * top], axis=0)
        value = times_columns(inverse_w, value)
        for k in block:
            work[k] = value[:, (k - j) * width : (k - j + 1) * width]

    rim = jnp.zeros((HALO, width), jnp.float32)
    field[:HALO, :] = rim
    field[HALO + length // 2 :, :] = rim

    def back(index, carry):
        base = pl.multiple_of(index * 8, 8)
        low = pl.ds(base, 8)
        high = pl.ds(pl.multiple_of(base + LANES, 8), 8)
        turn = table[low, :]
        spectrum = [(work[0, low, :], None)]
        for j in range(1, half):
            c = turn[:, j : j + 1]
            s = turn[:, half + j : half + j + 1]
            re, im = work[j, low, :], work[j, high, :]
            spectrum.append((re * c - im * s, re * s + im * c))
        spectrum.append((work[0, high, :], None))
        values = irfft(spectrum, factor)
        for a in range(half):
            field[pl.ds(pl.multiple_of(base + HALO + LANES * a, 8), 8), :] = values[a]
        return carry

    lax.fori_loop(0, LANES // 8, back, 0, unroll=4)
    for part in range(out.shape[0] // extent):
        begin = HALO - ABOVE + field_rows * part
        out[extent * part : extent * (part + 1), :] = field[begin : begin + extent, :]


def column_filter(column, scale, wave, tables, parts, field_rows):
    factor, _, width = column.shape
    length = factor * LANES
    vmem = pl.BlockSpec(memory_space=pltpu.VMEM)
    return pl.pallas_call(
        functools.partial(column_kernel, field_rows=field_rows),
        in_specs=[pl.BlockSpec(memory_space=pltpu.SMEM)] + [vmem] * 7,
        out_specs=vmem,
        out_shape=pltpu.HBM((parts * (field_rows + ABOVE + BELOW), width), jnp.float32),
        scratch_shapes=[
            pltpu.VMEM((factor // 2, 2 * LANES, width), jnp.float32),
            pltpu.VMEM((length // 2 + 2 * HALO, width), jnp.float32),
        ],
        compiler_params=pltpu.CompilerParams(vmem_limit_bytes=24 << 20),
        name="column_filter",
    )(scale, near(column), *tables, wave)


def observe_kernel(local, cells, values, count, total, left):
    rows, columns = count.shape
    block = columns
    origin = pl.program_id(0) * block

    @pl.when(pl.program_id(0) == 0)
    def _():
        row = lax.broadcasted_iota(jnp.int32, (rows, local.shape[1]), 0)
        here = row == local[...]
        value = jnp.broadcast_to(values[...], here.shape)
        first = value.astype(jnp.bfloat16).astype(jnp.float32)
        second = (value - first).astype(jnp.bfloat16).astype(jnp.float32)
        third = value - first - second
        for slot, piece in enumerate((1.0, first, second, third)):
            left[slot * rows : (slot + 1) * rows, :] = jnp.where(here, piece, 0.0).astype(jnp.bfloat16)

    spot = lax.broadcasted_iota(jnp.int32, (block, local.shape[1]), 0) + origin
    right = jnp.where(spot == cells[...], 1.0, 0.0).astype(jnp.bfloat16)
    result = lax.dot_general(
        left[...], right, (((1,), (1,)), ((), ())), preferred_element_type=jnp.float32
    )
    count[...] = result[:rows]
    total[...] = (result[3 * rows :] + result[2 * rows : 3 * rows]) + result[rows : 2 * rows]


def observe(local_row, cell_col, values, rows, columns):
    number = values.shape[1]
    block = 256
    whole = pl.BlockSpec((1, number), lambda i: (0, 0))
    piece = pl.BlockSpec((rows, block), lambda i: (0, i))
    shape = jax.ShapeDtypeStruct((rows, columns), jnp.float32)
    return pl.pallas_call(
        observe_kernel,
        compiler_params=pltpu.CompilerParams(vmem_limit_bytes=32 << 20),
        grid=(columns // block,),
        in_specs=[whole, whole, whole],
        out_specs=(piece, piece),
        out_shape=(shape, shape),
        scratch_shapes=[pltpu.VMEM((4 * rows, number), jnp.bfloat16)],
        cost_estimate=pl.CostEstimate(
            flops=8 * rows * number * columns, transcendentals=0, bytes_accessed=8 * rows * columns
        ),
        name="observe",
    )(local_row, cell_col, values)


def two_sum(a, b):
    s = a + b
    t = s - a
    return s, (a - (s - t)) + (b - t)


def split(a):
    t = a * 4097.0
    high = t - (t - a)
    return high, a - high


def two_prod(a, b):
    p = a * b
    ah, al = split(a)
    bh, bl = split(b)
    return p, ((ah * bh - p) + ah * bl + al * bh) + al * bl


def dd_add(x, y):
    s, e = two_sum(x[0], y[0])
    e = e + (x[1] + y[1])
    high = s + e
    return high, e - (high - s)


def dd_neg(x):
    return -x[0], -x[1]


def dd_mul(x, y):
    p, e = two_prod(x[0], y[0])
    e = e + (x[0] * y[1] + x[1] * y[0])
    high = p + e
    return high, e - (high - p)


def dd_div(x, y):
    first = x[0] / y[0]
    rest = dd_add(x, dd_neg(dd_mul(y, (first, jnp.zeros_like(first)))))
    second = rest[0] / y[0]
    rest = dd_add(rest, dd_neg(dd_mul(y, (second, jnp.zeros_like(first)))))
    third = rest[0] / y[0]
    high, low = two_sum(first, second)
    return dd_add((high, low), (third, jnp.zeros_like(third)))


def fold(high, low, shift, axis):
    other, error = two_sum(high, pltpu.roll(high, shift, axis))
    return other, (low + pltpu.roll(low, shift, axis)) + error


def fold_rows(value):
    pieces = [value[8 * i : 8 * i + 8] for i in range(value.shape[0] // 8)]
    while len(pieces) > 1:
        last = [pieces[-1]] if len(pieces) % 2 else []
        pieces = [a + b for a, b in zip(pieces[0::2], pieces[1::2])] + last
    return pieces[0]


def krylov_kernel(
    origin, coefs, source_hbm, count_hbm, total_hbm, twiddle, inverse_w, special_i,
    log_perm_hbm, basis, partial,
    received, work, kappa, centre, inverse, north, west, east, vector,
    source, count, total, log_perm, arrive, leave,
):
    inward = [
        pltpu.make_async_copy(far_ref, near_ref, arrive.at[k])
        for k, (far_ref, near_ref) in enumerate(
            ((source_hbm, source), (count_hbm, count), (total_hbm, total))
        )
    ]
    outward = pltpu.make_async_copy(log_perm, log_perm_hbm, leave)
    for copy in inward:
        copy.start()
    half, area, _ = work.shape
    factor = 2 * half
    rows = area - 2 * HALO
    extent = rows + ABOVE + BELOW
    groups = area // 8

    size = coefs.shape[0]
    rim = jnp.zeros((8, LANES), jnp.float32)
    received[:8, :] = rim
    received[8 + size : 16 + size, :] = rim
    received[8 : 8 + size, :] = coefs[...]

    def window(tile):
        begin = 8 + extent * tile + ABOVE - HALO
        return received[begin : begin + area, :]

    def pair(j):
        return jnp.concatenate([window(2 * j), window(2 * j + 1)], axis=1)

    work[0] = rows_times(pair(0), special_i)
    batch = 3
    for j in range(1, half, batch):
        value = rows_times(jnp.concatenate([pair(k) for k in range(j, j + batch)], axis=0), inverse_w)
        for k in range(batch):
            work[j + k] = value[k * area : (k + 1) * area]

    for tile in range(half):
        for ref in (kappa, vector.at[0], vector.at[1]):
            ref[tile, :8, :] = rim
            ref[tile, 8 + area :, :] = rim

    first_row = origin[0] - HALO
    limit = origin[1]

    def usable(start, count):
        local = lax.broadcasted_iota(jnp.int32, (count, LANES), 0) + start
        row = local + first_row
        inner = (local >= HALO - ABOVE) & (local < HALO + rows + BELOW)
        return inner & (row >= 0) & (row < limit)

    def inverse_group(index, carry):
        base = pl.multiple_of(index * 8, 8)
        low = pl.ds(base, 8)
        spectrum = [(work[0, low, :LANES], None)]
        for j in range(1, half):
            c = twiddle[j : j + 1, :]
            s = twiddle[half + j : half + j + 1, :]
            re, im = work[j, low, :LANES], work[j, low, LANES:]
            spectrum.append((re * c - im * s, re * s + im * c))
        spectrum.append((work[0, low, LANES:], None))
        values = irfft(spectrum, factor)
        valid = usable(base, 8)
        store = pl.ds(pl.multiple_of(base + 8, 8), 8)
        for a in range(half):
            kappa[a, store, :] = jnp.where(valid, 0.5 * jnp.exp(values[a]), 0.0)

        @pl.when((index >= HALO // 8) & (index < groups - HALO // 8))
        def _():
            own = pl.ds(pl.multiple_of(base - HALO, 8), 8)
            for a in range(half):
                log_perm[own, LANES * a : LANES * (a + 1)] = values[a]

        return carry

    lax.fori_loop(0, groups, inverse_group, 0, unroll=2)
    outward.start()
    inward[0].wait()

    first_lane = lax.broadcasted_iota(jnp.int32, (1, LANES), 1) == 0
    last_lane = lax.broadcasted_iota(jnp.int32, (1, LANES), 1) == LANES - 1
    sums = [rim] * SUMS
    own = slice(HALO, HALO + rows)
    every = slice(8, 8 + area)
    before = slice(7, 7 + area)
    after = slice(9, 9 + area)

    def sideways(load):
        back, ahead = None, None
        value = load(0)
        for tile in range(half):
            following = load(tile + 1) if tile + 1 < half else None
            turned = pltpu.roll(value, 1, 1)
            ahead = pltpu.roll(value, LANES - 1, 1) if tile == 0 else ahead
            left = jnp.where(first_lane, 0.0 if back is None else back, turned)
            if following is None:
                right = jnp.where(last_lane, 0.0, ahead)
            else:
                next_ahead = pltpu.roll(following, LANES - 1, 1)
                right = jnp.where(last_lane, next_ahead, ahead)
                ahead = next_ahead
            yield tile, value, left, right
            back, value = turned, following

    valid = usable(0, area)
    for tile, here, left, right in sideways(lambda t: kappa[t, every, :]):
        lanes = slice(LANES * tile, LANES * (tile + 1))
        up = here + kappa[tile, before, :]
        down = here + kappa[tile, after, :]
        left = here + left
        right = here + right
        middle = up + down + left + right
        rest = jnp.where(valid, 1.0 / middle, 0.0)
        centre[tile] = middle
        inverse[tile] = rest
        north[tile, :area, :] = up
        north[tile, area:, :] = rim
        west[tile] = left
        east[tile] = right
        first = source[:, lanes]
        value = first * rest
        vector[0, tile, every, :] = value
        basis[0, :, lanes] = value[own]
        sums[0] = sums[0] + fold_rows((first * value)[own])

    for step in range(ITERS - 1):
        now = vector.at[step % 2]
        new = vector.at[(step + 1) % 2]
        for tile, here, left, right in sideways(lambda t: now[t, every, :]):
            image = (
                centre[tile] * here
                - north[tile, :area, :] * now[tile, before, :]
                - north[tile, 1 : area + 1, :] * now[tile, after, :]
                - west[tile] * left
                - east[tile] * right
            )
            value = image * inverse[tile]
            new[tile, every, :] = value
            basis[step + 1, :, LANES * tile : LANES * (tile + 1)] = value[own]
            sums[2 * step + 1] = sums[2 * step + 1] + fold_rows((here * image)[own])
            sums[2 * step + 2] = sums[2 * step + 2] + fold_rows((value * image)[own])

    inward[1].wait()
    inward[2].wait()
    now = vector.at[(ITERS - 1) % 2]
    back = None
    for tile in range(half):
        lanes = slice(LANES * tile, LANES * (tile + 1))
        here = now[tile, 8 + HALO : 8 + HALO + rows, :]
        turned = pltpu.roll(here, 1, 1)
        left = jnp.where(first_lane, 0.0 if back is None else back, turned)
        back = turned
        shared = (
            north[tile, HALO + 1 : HALO + 1 + rows, :] * now[tile, 9 + HALO : 9 + HALO + rows, :]
            + west[tile, own, :] * left
        )
        energy = here * (centre[tile, own, :] * here - 2.0 * shared)
        sums[TERMS - 1] = sums[TERMS - 1] + fold_rows(energy)
        vectors = [basis[k, :, lanes] for k in range(ITERS)]
        weight = count[:, lanes]
        weighted = [weight * v for v in vectors]
        for spot, (i, j) in enumerate(PAIRS):
            sums[TERMS + spot] = sums[TERMS + spot] + fold_rows(weighted[i] * vectors[j])
        datum = total[:, lanes]
        for k in range(ITERS):
            slot = TERMS + len(PAIRS) + k
            sums[slot] = sums[slot] + fold_rows(datum * vectors[k])

    sub = lax.broadcasted_iota(jnp.int32, (8, LANES), 0)
    spot = lax.broadcasted_iota(jnp.int32, (8, LANES), 1)
    row = rim
    for begin in range(0, SUMS, 8):
        high, low = rim, rim
        for k in range(begin, min(begin + 8, SUMS)):
            h, e = sums[k], rim
            for shift in (4, 2, 1):
                h, e = fold(h, e, shift, 0)
            high = jnp.where(sub == k - begin, h, high)
            low = jnp.where(sub == k - begin, e, low)
        for shift in (64, 32, 16, 8, 4, 2, 1):
            high, low = fold(high, low, shift, 1)
        row = row + jnp.where(spot == sub + begin, high, 0.0)
        row = row + jnp.where(spot == sub + begin + LANES // 2, low, 0.0)
    for shift in (4, 2, 1):
        row = row + pltpu.roll(row, shift, 0)
    for part in range(partial.shape[0]):
        partial[part] = row[:1]
    outward.wait()


def krylov(origin, coefs, source, count, total, tables, parts):
    area, columns = source.shape
    half = columns // LANES
    rows = area - 2 * HALO
    vmem = pl.BlockSpec(memory_space=pltpu.VMEM)
    anywhere = pl.BlockSpec(memory_space=pl.ANY)
    plane = pltpu.VMEM((half, area, LANES), jnp.float32)
    padded = pltpu.VMEM((half, area + 16, LANES), jnp.float32)
    strip = pltpu.VMEM((rows, columns), jnp.float32)
    return pl.pallas_call(
        krylov_kernel,
        in_specs=[pl.BlockSpec(memory_space=pltpu.SMEM), vmem] + [anywhere] * 3 + [vmem] * 3,
        out_specs=(anywhere, vmem, vmem),
        out_shape=(
            pltpu.HBM((rows, columns), jnp.float32),
            pltpu.VMEM((ITERS, rows, columns), jnp.float32),
            pltpu.VMEM((parts, 1, LANES), jnp.float32),
        ),
        scratch_shapes=[
            pltpu.VMEM((coefs.shape[0] + 16, LANES), jnp.float32),
            pltpu.VMEM((half, area, 2 * LANES), jnp.float32),
            padded,
            plane,
            plane,
            pltpu.VMEM((half, area + 8, LANES), jnp.float32),
            plane,
            plane,
            pltpu.VMEM((2, half, area + 16, LANES), jnp.float32),
            pltpu.VMEM((area, columns), jnp.float32),
            strip,
            strip,
            strip,
            pltpu.SemaphoreType.DMA((3,)),
            pltpu.SemaphoreType.DMA(()),
        ],
        compiler_params=pltpu.CompilerParams(vmem_limit_bytes=32 << 20),
        name="krylov",
    )(origin, near(coefs), far(source), far(count), far(total), *tables)


def final_kernel(partial, basis, values, pressure, loglik):
    parts = partial.shape[0]
    high = jnp.concatenate([partial[k] for k in range(parts)], axis=0)
    low = pltpu.roll(high, LANES // 2, 1)
    while high.shape[0] > 8:
        middle = high.shape[0] // 2
        top, error = two_sum(high[:middle], high[middle:])
        low = (low[:middle] + low[middle:]) + error
        high = top
    for shift in (4, 2, 1):
        high, low = fold(high, low, shift, 0)

    def pick(k):
        return (
            jnp.broadcast_to(high[:, k : k + 1], (8, LANES)),
            jnp.broadcast_to(low[:, k : k + 1], (8, LANES)),
        )

    moments = [pick(k) for k in range(TERMS)]
    matrix = [[moments[i + j + 1] for j in range(ITERS)] for i in range(ITERS)]
    right = [moments[i] for i in range(ITERS)]
    for i in range(ITERS):
        for r in range(i + 1, ITERS):
            ratio = dd_neg(dd_div(matrix[i][r], matrix[i][i]))
            for c in range(r, ITERS):
                matrix[r][c] = dd_add(matrix[r][c], dd_mul(ratio, matrix[i][c]))
            right[r] = dd_add(right[r], dd_mul(ratio, right[i]))
    weights = [None] * ITERS
    for i in reversed(range(ITERS)):
        value = right[i]
        for c in range(i + 1, ITERS):
            value = dd_add(value, dd_neg(dd_mul(matrix[i][c], weights[c])))
        weights[i] = dd_div(value, matrix[i][i])

    data = values[...]
    h, e = two_prod(data, data)
    while h.shape[0] > 8:
        middle = h.shape[0] // 2
        top, error = two_sum(h[:middle], h[middle:])
        e = (e[:middle] + e[middle:]) + error
        h = top
    for shift in (4, 2, 1):
        h, e = fold(h, e, shift, 0)
    for shift in (64, 32, 16, 8, 4, 2, 1):
        h, e = fold(h, e, shift, 1)
    misfit = (h, e)
    for spot, (i, j) in enumerate(PAIRS):
        term = dd_mul(dd_mul(weights[i], weights[j]), pick(TERMS + spot))
        misfit = dd_add(misfit, term)
        if i != j:
            misfit = dd_add(misfit, term)
    for k in range(ITERS):
        term = dd_neg(dd_mul(weights[k], pick(TERMS + len(PAIRS) + k)))
        misfit = dd_add(misfit, dd_add(term, term))
    number = values.shape[0] * LANES
    loglik[...] = (-(2.0 / number) * (misfit[0] + misfit[1]))[:1, :]

    factors = [w[0][:1, :1] for w in weights]
    for group in range(pressure.shape[0] // 8):
        put = slice(8 * group, 8 * group + 8)
        value = factors[0] * basis[0, put, :]
        for k in range(1, ITERS):
            value = value + factors[k] * basis[k, put, :]
        pressure[put, :] = value


def finish(partial, basis, values):
    vmem = pl.BlockSpec(memory_space=pltpu.VMEM)
    return pl.pallas_call(
        final_kernel,
        in_specs=[vmem] * 3,
        out_specs=(vmem, vmem),
        out_shape=(
            jax.ShapeDtypeStruct(basis.shape[1:], jnp.float32),
            jax.ShapeDtypeStruct((1, LANES), jnp.float32),
        ),
        compiler_params=pltpu.CompilerParams(vmem_limit_bytes=16 << 20),
        name="finish",
    )(near(partial), near(basis), near(values))


def exchange(block):
    return lax.all_to_all(block, "strip", split_axis=0, concat_axis=0, tiled=True)


def body(state, noise, step, field_scale, wave_scale, source, obs_cells, obs_values):
    parts = lax.axis_size("strip")
    position = lax.axis_index("strip")
    rows_here, length = state.shape
    factor = length // LANES
    half = factor // 2
    width = length // parts
    ways = parts // factor
    field_rows, columns = source.shape

    forward, inverse, special_f, special_i = dft_tables()
    cos, sin = twiddle_table(length, factor)
    across = np.float32(np.concatenate([cos, sin], 0))
    down = np.zeros((LANES, LANES), np.float32)
    down[:, :factor] = across.T

    ahead = [(i, i + 1) for i in range(parts - 1)]
    behind = [(b, a) for a, b in ahead]
    above = lax.ppermute(source[field_rows - HALO :], "strip", ahead)
    below = lax.ppermute(source[:HALO], "strip", behind)
    wide_source = jnp.concatenate([above, source, below], axis=0)

    cell_row = obs_cells // columns - position * field_rows
    count, total = observe(
        cell_row[None, :], (obs_cells % columns)[None, :], obs_values[None, :], field_rows, columns
    )

    tiles = row_forward(state, noise, step, (across, pieces(forward), pieces(special_f)))
    if ways > 1:
        tiles = tiles.reshape(factor, rows_here, ways, width).transpose(0, 2, 1, 3)
        tiles = tiles.reshape(parts, rows_here, width)
    column = exchange(tiles).reshape(factor, LANES, width)

    slot = position * width + lax.broadcasted_iota(jnp.int32, (1, width), 1)
    tile, lane = slot // LANES, slot % LANES
    middle = LANES // 2
    freq = jnp.where(
        tile == 0,
        factor * jnp.where(lane > middle, lane - middle, lane),
        jnp.where(
            tile == 1,
            half + factor * jnp.where(lane >= middle, lane - middle, lane),
            tile // 2 + factor * lane,
        ),
    )
    freq = jnp.minimum(freq, length - freq).astype(jnp.float32)
    wave = wave_scale[0]
    gain = field_scale[0] * wave / (math.sqrt(math.pi) * length)
    scale = jnp.stack([gain, wave * wave])
    blocks = column_filter(
        column,
        scale,
        freq * freq,
        (down, *(pieces(t.T) for t in (forward, special_f, inverse, special_i))),
        parts,
        field_rows,
    )
    extent = field_rows + ABOVE + BELOW
    coefs = exchange(blocks.reshape(parts, 1, extent * width))
    if ways > 1:
        coefs = coefs.reshape(factor, ways, extent, width).transpose(0, 2, 1, 3)
    coefs = coefs.reshape(factor * extent, LANES)

    origin = jnp.stack([position * field_rows, parts * field_rows]).astype(jnp.int32)
    log_perm, basis, partial = krylov(
        origin, coefs, wide_source, count, total, (across, pieces(inverse), pieces(special_i)), parts
    )
    pressure, loglik = finish(exchange(partial), basis, obs_values.reshape(-1, LANES))
    return (log_perm, pressure, loglik[0, 0])


def solution(mesh):
    placed = (P("strip", None), P("strip", None), P(), P(), P(), P("strip", None), P(), P())
    return jax.shard_map(
        body,
        mesh=mesh,
        in_specs=placed,
        out_specs=(P("strip", None), P("strip", None), P()),
        check_vma=False,
    )
```

```python
import functools
import math

import jax
import jax.numpy as jnp
import numpy as np
from jax import lax
from jax.experimental import pallas as pl
from jax.experimental.pallas import tpu as pltpu
from jax.sharding import PartitionSpec as P

ITERS = 4
LANES = 128
HALO = 8
ABOVE = ITERS
BELOW = ITERS + 1
TERMS = 2 * ITERS
PAIRS = [(i, j) for i in range(ITERS) for j in range(i, ITERS)]
SUMS = TERMS + len(PAIRS) + ITERS


def dot(left, right):
    return lax.dot_general(
        left, right, (((1,), (0,)), ((), ())), preferred_element_type=jnp.float32
    )


def halves(value):
    high = value.astype(jnp.bfloat16)
    return high, (value - high.astype(jnp.float32)).astype(jnp.bfloat16)


def rows_times(value, table):
    size = value.shape[1]
    high, low = halves(value)
    upper = table[:size, :]
    return dot(high, table[size:, :]) + dot(low, upper) + dot(high, upper)


def times_columns(table, value):
    size = value.shape[0]
    high, low = halves(value)
    upper = table[:size, :]
    return dot(table[size:, :], high) + dot(upper, low) + dot(upper, high)


def pieces(table):
    table = np.asarray(table, np.float64)
    high = table.astype(jnp.bfloat16)
    low = (table - high.astype(np.float64)).astype(jnp.bfloat16)
    return np.concatenate([high, low], 0)


def near(value):
    return pltpu.with_memory_space_constraint(value, pltpu.VMEM)


def far(value):
    return pltpu.with_memory_space_constraint(value, pltpu.HBM)


def dft_tables():
    spot = np.arange(LANES)
    angle = 2.0 * np.pi * np.outer(spot, spot) / LANES
    cos, sin = np.cos(angle), np.sin(angle)
    forward = np.block([[cos, -sin], [sin, cos]])
    inverse = np.block([[cos, sin], [-sin, cos]])
    half = LANES // 2
    whole = 2.0 * np.pi * np.outer(spot, np.arange(1, half)) / LANES
    edge = np.ones((LANES, 1))
    alternate = ((-1.0) ** spot)[:, None]
    zero_f = np.concatenate([edge, np.cos(whole), alternate, -np.sin(whole)], 1)
    zero_i = np.concatenate([edge, 2 * np.cos(whole), alternate, -2 * np.sin(whole)], 1).T
    odd = 2.0 * np.pi * np.outer(spot, np.arange(half) + 0.5) / LANES
    half_f = np.concatenate([np.cos(odd), -np.sin(odd)], 1)
    half_i = 2.0 * np.concatenate([np.cos(odd), -np.sin(odd)], 1).T
    none = np.zeros((LANES, LANES))
    special_f = np.block([[zero_f, none], [none, half_f]])
    special_i = np.block([[zero_i, none], [none, half_i]])
    return forward, inverse, special_f, special_i


def twiddle_table(length, factor):
    angle = 2.0 * np.pi * np.outer(np.arange(factor // 2), np.arange(LANES)) / length
    return np.cos(angle), np.sin(angle)


def times(value, factor):
    if value is None or factor == 0.0:
        return None
    if factor == 1.0:
        return value
    if factor == -1.0:
        return -value
    return value * factor


def plus(left, right):
    if left is None:
        return right
    if right is None:
        return left
    return left + right


def minus(left, right):
    if right is None:
        return left
    if left is None:
        return -right
    return left - right


def root(k, n):
    quarter = (8 * k) % (8 * n)
    if quarter % n == 0 and (quarter // n) % 2 == 0:
        return ((1.0, 0.0), (0.0, 1.0), (-1.0, 0.0), (0.0, -1.0))[(quarter // n) // 2]
    return (math.cos(2 * math.pi * k / n), math.sin(2 * math.pi * k / n))


def rotate(re, im, c, s):
    return (
        minus(times(re, c), times(im, s)),
        plus(times(re, s), times(im, c)),
    )


def rfft(values):
    n = len(values)
    if n == 2:
        return [(values[0] + values[1], None), (values[0] - values[1], None)]
    even = rfft(values[0::2])
    odd = rfft(values[1::2])
    out = [None] * (n // 2 + 1)
    for k in range(n // 4 + 1):
        c, s = root(k, n)
        tr, ti = rotate(odd[k][0], odd[k][1], c, -s)
        er, ei = even[k]
        out[k] = (plus(er, tr), plus(ei, ti))
        if k != n // 4:
            out[n // 2 - k] = (minus(er, tr), minus(ti, ei))
    return out


def irfft(spectrum, n):
    if n == 2:
        return [spectrum[0][0] + spectrum[1][0]]
    even, odd = [], []
    for k in range(n // 4 + 1):
        ar, ai = spectrum[k]
        br, bi = spectrum[n // 2 - k]
        if k == n // 4:
            even.append((2.0 * ar, None))
            odd.append((-2.0 * ai, None))
            continue
        even.append((plus(ar, br), minus(ai, bi)))
        c, s = root(k, n)
        odd.append(rotate(minus(ar, br), plus(ai, bi), c, s))
    even = irfft(even, n // 2)
    odd = irfft(odd, n // 2)
    return [value for pair in zip(even, odd) for value in pair]


def row_kernel(step, state, noise, twiddle, pair_w, special_w, out, work, *, factor):
    rows = state.shape[0]
    half = factor // 2
    rate = step[0]
    keep = jnp.sqrt(jnp.full((8, LANES), 1.0 - rate * rate, jnp.float32))

    def group(index, carry):
        base = pl.multiple_of(index * 8, 8)
        tiles = [
            keep * state[pl.ds(base, 8), LANES * a : LANES * (a + 1)]
            + rate * noise[pl.ds(base, 8), LANES * a : LANES * (a + 1)]
            for a in range(factor)
        ]
        spectrum = rfft(tiles)
        work[0, pl.ds(base, 8), :LANES] = spectrum[0][0]
        work[0, pl.ds(base, 8), LANES:] = spectrum[half][0]
        for j in range(1, half):
            c = twiddle[j : j + 1, :]
            s = twiddle[half + j : half + j + 1, :]
            re, im = spectrum[j]
            work[j, pl.ds(base, 8), :LANES] = re * c + im * s
            work[j, pl.ds(base, 8), LANES:] = im * c - re * s
        return carry

    lax.fori_loop(0, rows // 8, group, 0, unroll=4)
    put = slice(None)
    first = rows_times(work[0], special_w)
    out[0, put, :] = first[:, :LANES]
    out[1, put, :] = first[:, LANES:]
    batch = 5
    for begin in range(1, half, batch):
        value = rows_times(work[begin : begin + batch].reshape(batch * rows, 2 * LANES), pair_w)
        for k in range(batch):
            out[2 * (begin + k), put, :] = value[k * rows : (k + 1) * rows, :LANES]
            out[2 * (begin + k) + 1, put, :] = value[k * rows : (k + 1) * rows, LANES:]


def row_forward(state, noise, step, tables):
    rows, length = state.shape
    factor = length // LANES
    block = min(64, rows)
    twiddle, pair_w, special_w = tables
    whole = lambda i: (0, 0)
    return pl.pallas_call(
        functools.partial(row_kernel, factor=factor),
        grid=(rows // block,),
        in_specs=[
            pl.BlockSpec(memory_space=pltpu.SMEM),
            pl.BlockSpec((block, length), lambda i: (i, 0)),
            pl.BlockSpec((block, length), lambda i: (i, 0)),
            pl.BlockSpec(twiddle.shape, whole),
            pl.BlockSpec(pair_w.shape, whole),
            pl.BlockSpec(special_w.shape, whole),
        ],
        out_specs=pl.BlockSpec((factor, block, LANES), lambda i: (0, i, 0)),
        out_shape=pltpu.HBM((factor, rows, LANES), jnp.float32),
        scratch_shapes=[pltpu.VMEM((factor // 2, block, 2 * LANES), jnp.float32)],
        compiler_params=pltpu.CompilerParams(vmem_limit_bytes=16 << 20),
        name="row_forward",
    )(step, far(state), far(noise), far(twiddle), far(pair_w), far(special_w))


def column_kernel(
    scale, column, table, forward_w, special_f, inverse_w, special_i, wave, out, work, field, *, field_rows
):
    factor, _, width = column.shape
    half = factor // 2
    length = factor * LANES
    extent = field_rows + ABOVE + BELOW

    def ahead(index, carry):
        base = pl.multiple_of(index * 8, 8)
        spectrum = rfft([column[a, pl.ds(base, 8), :] for a in range(factor)])
        low = pl.ds(base, 8)
        high = pl.ds(pl.multiple_of(base + LANES, 8), 8)
        work[0, low, :] = spectrum[0][0]
        work[0, high, :] = spectrum[half][0]
        turn = table[low, :]
        for j in range(1, half):
            c = turn[:, j : j + 1]
            s = turn[:, half + j : half + j + 1]
            re, im = spectrum[j]
            work[j, low, :] = re * c + im * s
            work[j, high, :] = im * c - re * s
        return carry

    lax.fori_loop(0, LANES // 8, ahead, 0, unroll=4)
    place = lax.broadcasted_iota(jnp.int32, (LANES, width), 0)
    side = wave[...] + scale[1]
    gain = scale[0]

    def amplitude(freq):
        freq = jnp.minimum(freq, length - freq).astype(jnp.float32)
        return gain / (freq * freq + side)

    batch = 2 if width % LANES == 0 else 1
    for j in range(half):
        if j == 0:
            value = times_columns(special_f, work[0])
            middle = LANES // 2
            top = amplitude(factor * jnp.where(place > middle, place - middle, place))
            low = amplitude(half + factor * jnp.where(place >= middle, place - middle, place))
            value = jnp.concatenate([value[:LANES] * top, value[LANES:] * low], axis=0)
            work[0] = times_columns(special_i, value)
            continue
        if (j - 1) % batch:
            continue
        block = range(j, min(j + batch, half))
        value = times_columns(forward_w, jnp.concatenate([work[k] for k in block], axis=1))
        top = jnp.concatenate([amplitude(k + factor * place) for k in block], axis=1)
        value = jnp.concatenate([value[:LANES] * top, value[LANES:] * top], axis=0)
        value = times_columns(inverse_w, value)
        for k in block:
            work[k] = value[:, (k - j) * width : (k - j + 1) * width]

    rim = jnp.zeros((HALO, width), jnp.float32)
    field[:HALO, :] = rim
    field[HALO + length // 2 :, :] = rim

    def back(index, carry):
        base = pl.multiple_of(index * 8, 8)
        low = pl.ds(base, 8)
        high = pl.ds(pl.multiple_of(base + LANES, 8), 8)
        turn = table[low, :]
        spectrum = [(work[0, low, :], None)]
        for j in range(1, half):
            c = turn[:, j : j + 1]
            s = turn[:, half + j : half + j + 1]
            re, im = work[j, low, :], work[j, high, :]
            spectrum.append((re * c - im * s, re * s + im * c))
        spectrum.append((work[0, high, :], None))
        values = irfft(spectrum, factor)
        for a in range(half):
            field[pl.ds(pl.multiple_of(base + HALO + LANES * a, 8), 8), :] = values[a]
        return carry

    lax.fori_loop(0, LANES // 8, back, 0, unroll=4)
    for part in range(out.shape[0] // extent):
        begin = HALO - ABOVE + field_rows * part
        out[extent * part : extent * (part + 1), :] = field[begin : begin + extent, :]


def column_filter(column, scale, wave, tables, parts, field_rows):
    factor, _, width = column.shape
    length = factor * LANES
    vmem = pl.BlockSpec(memory_space=pltpu.VMEM)
    return pl.pallas_call(
        functools.partial(column_kernel, field_rows=field_rows),
        in_specs=[pl.BlockSpec(memory_space=pltpu.SMEM)] + [vmem] * 7,
        out_specs=vmem,
        out_shape=pltpu.HBM((parts * (field_rows + ABOVE + BELOW), width), jnp.float32),
        scratch_shapes=[
            pltpu.VMEM((factor // 2, 2 * LANES, width), jnp.float32),
            pltpu.VMEM((length // 2 + 2 * HALO, width), jnp.float32),
        ],
        compiler_params=pltpu.CompilerParams(vmem_limit_bytes=24 << 20),
        name="column_filter",
    )(scale, near(column), *tables, wave)


def observe_kernel(local, cells, values, count, total, left):
    rows, columns = count.shape
    block = columns
    origin = pl.program_id(0) * block

    @pl.when(pl.program_id(0) == 0)
    def _():
        row = lax.broadcasted_iota(jnp.int32, (rows, local.shape[1]), 0)
        here = row == local[...]
        value = jnp.broadcast_to(values[...], here.shape)
        first = value.astype(jnp.bfloat16).astype(jnp.float32)
        second = (value - first).astype(jnp.bfloat16).astype(jnp.float32)
        third = value - first - second
        for slot, piece in enumerate((1.0, first, second, third)):
            left[slot * rows : (slot + 1) * rows, :] = jnp.where(here, piece, 0.0).astype(jnp.bfloat16)

    spot = lax.broadcasted_iota(jnp.int32, (block, local.shape[1]), 0) + origin
    right = jnp.where(spot == cells[...], 1.0, 0.0).astype(jnp.bfloat16)
    result = lax.dot_general(
        left[...], right, (((1,), (1,)), ((), ())), preferred_element_type=jnp.float32
    )
    count[...] = result[:rows]
    total[...] = (result[3 * rows :] + result[2 * rows : 3 * rows]) + result[rows : 2 * rows]


def observe(local_row, cell_col, values, rows, columns):
    number = values.shape[1]
    block = 256
    whole = pl.BlockSpec((1, number), lambda i: (0, 0))
    piece = pl.BlockSpec((rows, block), lambda i: (0, i))
    shape = jax.ShapeDtypeStruct((rows, columns), jnp.float32)
    return pl.pallas_call(
        observe_kernel,
        compiler_params=pltpu.CompilerParams(vmem_limit_bytes=32 << 20),
        grid=(columns // block,),
        in_specs=[whole, whole, whole],
        out_specs=(piece, piece),
        out_shape=(shape, shape),
        scratch_shapes=[pltpu.VMEM((4 * rows, number), jnp.bfloat16)],
        cost_estimate=pl.CostEstimate(
            flops=8 * rows * number * columns, transcendentals=0, bytes_accessed=8 * rows * columns
        ),
        name="observe",
    )(local_row, cell_col, values)


def two_sum(a, b):
    s = a + b
    t = s - a
    return s, (a - (s - t)) + (b - t)


def split(a):
    t = a * 4097.0
    high = t - (t - a)
    return high, a - high


def two_prod(a, b):
    p = a * b
    ah, al = split(a)
    bh, bl = split(b)
    return p, ((ah * bh - p) + ah * bl + al * bh) + al * bl


def dd_add(x, y):
    s, e = two_sum(x[0], y[0])
    e = e + (x[1] + y[1])
    high = s + e
    return high, e - (high - s)


def dd_neg(x):
    return -x[0], -x[1]


def dd_mul(x, y):
    p, e = two_prod(x[0], y[0])
    e = e + (x[0] * y[1] + x[1] * y[0])
    high = p + e
    return high, e - (high - p)


def dd_div(x, y):
    first = x[0] / y[0]
    rest = dd_add(x, dd_neg(dd_mul(y, (first, jnp.zeros_like(first)))))
    second = rest[0] / y[0]
    rest = dd_add(rest, dd_neg(dd_mul(y, (second, jnp.zeros_like(first)))))
    third = rest[0] / y[0]
    high, low = two_sum(first, second)
    return dd_add((high, low), (third, jnp.zeros_like(third)))


def fold(high, low, shift, axis):
    other, error = two_sum(high, pltpu.roll(high, shift, axis))
    return other, (low + pltpu.roll(low, shift, axis)) + error


def fold_rows(value):
    pieces = [value[8 * i : 8 * i + 8] for i in range(value.shape[0] // 8)]
    while len(pieces) > 1:
        last = [pieces[-1]] if len(pieces) % 2 else []
        pieces = [a + b for a, b in zip(pieces[0::2], pieces[1::2])] + last
    return pieces[0]


def krylov_kernel(
    origin, coefs, source_hbm, count_hbm, total_hbm, twiddle, inverse_w, special_i,
    log_perm_hbm, basis, partial,
    received, work, kappa, inverse, north, south, west, east, vector,
    source, count, total, log_perm, arrive, leave,
):
    inward = [
        pltpu.make_async_copy(far_ref, near_ref, arrive.at[k])
        for k, (far_ref, near_ref) in enumerate(
            ((source_hbm, source), (count_hbm, count), (total_hbm, total))
        )
    ]
    outward = pltpu.make_async_copy(log_perm, log_perm_hbm, leave)
    for copy in inward:
        copy.start()
    half, area, _ = work.shape
    factor = 2 * half
    rows = area - 2 * HALO
    extent = rows + ABOVE + BELOW
    groups = area // 8

    size = coefs.shape[0]
    rim = jnp.zeros((8, LANES), jnp.float32)
    received[:8, :] = rim
    received[8 + size : 16 + size, :] = rim
    received[8 : 8 + size, :] = coefs[...]

    def window(tile):
        begin = 8 + extent * tile + ABOVE - HALO
        return received[begin : begin + area, :]

    def pair(j):
        return jnp.concatenate([window(2 * j), window(2 * j + 1)], axis=1)

    work[0] = rows_times(pair(0), special_i)
    batch = 3
    for j in range(1, half, batch):
        value = rows_times(jnp.concatenate([pair(k) for k in range(j, j + batch)], axis=0), inverse_w)
        for k in range(batch):
            work[j + k] = value[k * area : (k + 1) * area]

    for tile in range(half):
        for ref in (kappa, vector.at[0], vector.at[1]):
            ref[tile, :8, :] = rim
            ref[tile, 8 + area :, :] = rim

    first_row = origin[0] - HALO
    limit = origin[1]

    def usable(start, count):
        local = lax.broadcasted_iota(jnp.int32, (count, LANES), 0) + start
        row = local + first_row
        inner = (local >= HALO - ABOVE) & (local < HALO + rows + BELOW)
        return inner & (row >= 0) & (row < limit)

    def inverse_group(index, carry):
        base = pl.multiple_of(index * 8, 8)
        low = pl.ds(base, 8)
        spectrum = [(work[0, low, :LANES], None)]
        for j in range(1, half):
            c = twiddle[j : j + 1, :]
            s = twiddle[half + j : half + j + 1, :]
            re, im = work[j, low, :LANES], work[j, low, LANES:]
            spectrum.append((re * c - im * s, re * s + im * c))
        spectrum.append((work[0, low, LANES:], None))
        values = irfft(spectrum, factor)
        valid = usable(base, 8)
        store = pl.ds(pl.multiple_of(base + 8, 8), 8)
        for a in range(half):
            kappa[a, store, :] = jnp.where(valid, 0.5 * jnp.exp(values[a]), 0.0)

        @pl.when((index >= HALO // 8) & (index < groups - HALO // 8))
        def _():
            own = pl.ds(pl.multiple_of(base - HALO, 8), 8)
            for a in range(half):
                log_perm[own, LANES * a : LANES * (a + 1)] = values[a]

        return carry

    lax.fori_loop(0, groups, inverse_group, 0, unroll=2)
    outward.start()
    inward[0].wait()

    first_lane = lax.broadcasted_iota(jnp.int32, (1, LANES), 1) == 0
    last_lane = lax.broadcasted_iota(jnp.int32, (1, LANES), 1) == LANES - 1
    sums = [rim] * SUMS
    own = slice(HALO, HALO + rows)
    every = slice(8, 8 + area)
    before = slice(7, 7 + area)
    after = slice(9, 9 + area)

    def sideways(load):
        back, ahead = None, None
        value = load(0)
        for tile in range(half):
            following = load(tile + 1) if tile + 1 < half else None
            turned = pltpu.roll(value, 1, 1)
            ahead = pltpu.roll(value, LANES - 1, 1) if tile == 0 else ahead
            left = jnp.where(first_lane, 0.0 if back is None else back, turned)
            if following is None:
                right = jnp.where(last_lane, 0.0, ahead)
            else:
                next_ahead = pltpu.roll(following, LANES - 1, 1)
                right = jnp.where(last_lane, next_ahead, ahead)
                ahead = next_ahead
            yield tile, value, left, right
            back, value = turned, following

    valid = usable(0, area)
    for tile, here, left, right in sideways(lambda t: kappa[t, every, :]):
        lanes = slice(LANES * tile, LANES * (tile + 1))
        up = here + kappa[tile, before, :]
        down = here + kappa[tile, after, :]
        left = here + left
        right = here + right
        middle = up + down + left + right
        rest = jnp.where(valid, 1.0 / middle, 0.0)
        inverse[tile] = rest
        north[tile] = up
        south[tile] = down
        west[tile] = left
        east[tile] = right
        first = source[:, lanes]
        value = first * rest
        vector[0, tile, every, :] = value
        basis[0, :, lanes] = value[own]
        sums[0] = sums[0] + fold_rows((first * value)[own])

    for step in range(ITERS - 1):
        now = vector.at[step % 2]
        new = vector.at[(step + 1) % 2]
        for tile, here, left, right in sideways(lambda t: now[t, every, :]):
            image = (
                north[tile] * (here - now[tile, before, :])
                + south[tile] * (here - now[tile, after, :])
                + west[tile] * (here - left)
                + east[tile] * (here - right)
            )
            value = image * inverse[tile]
            new[tile, every, :] = value
            basis[step + 1, :, LANES * tile : LANES * (tile + 1)] = value[own]
            sums[2 * step + 1] = sums[2 * step + 1] + fold_rows((here * image)[own])
            sums[2 * step + 2] = sums[2 * step + 2] + fold_rows((value * image)[own])

    inward[1].wait()
    inward[2].wait()
    now = vector.at[(ITERS - 1) % 2]
    first = lax.broadcasted_iota(jnp.int32, (8, LANES), 0) + origin[0] == 0
    back = None
    for tile in range(half):
        lanes = slice(LANES * tile, LANES * (tile + 1))
        here = now[tile, 8 + HALO : 8 + HALO + rows, :]
        turned = pltpu.roll(here, 1, 1)
        left = jnp.where(first_lane, 0.0 if back is None else back, turned)
        back = turned
        down = here - now[tile, 9 + HALO : 9 + HALO + rows, :]
        across = here - left
        energy = fold_rows(south[tile, own, :] * (down * down) + west[tile, own, :] * (across * across))
        top = here[:8]
        energy = energy + jnp.where(first, north[tile, HALO : HALO + 8, :] * (top * top), 0.0)
        if tile == half - 1:
            energy = energy + fold_rows(jnp.where(last_lane, east[tile, own, :] * (here * here), 0.0))
        sums[TERMS - 1] = sums[TERMS - 1] + energy
        vectors = [basis[k, :, lanes] for k in range(ITERS)]
        weight = count[:, lanes]
        weighted = [weight * v for v in vectors]
        for spot, (i, j) in enumerate(PAIRS):
            sums[TERMS + spot] = sums[TERMS + spot] + fold_rows(weighted[i] * vectors[j])
        datum = total[:, lanes]
        for k in range(ITERS):
            slot = TERMS + len(PAIRS) + k
            sums[slot] = sums[slot] + fold_rows(datum * vectors[k])

    sub = lax.broadcasted_iota(jnp.int32, (8, LANES), 0)
    spot = lax.broadcasted_iota(jnp.int32, (8, LANES), 1)
    row = rim
    for begin in range(0, SUMS, 8):
        high, low = rim, rim
        for k in range(begin, min(begin + 8, SUMS)):
            h, e = sums[k], rim
            for shift in (4, 2, 1):
                h, e = fold(h, e, shift, 0)
            high = jnp.where(sub == k - begin, h, high)
            low = jnp.where(sub == k - begin, e, low)
        for shift in (64, 32, 16, 8, 4, 2, 1):
            high, low = fold(high, low, shift, 1)
        row = row + jnp.where(spot == sub + begin, high, 0.0)
        row = row + jnp.where(spot == sub + begin + LANES // 2, low, 0.0)
    for shift in (4, 2, 1):
        row = row + pltpu.roll(row, shift, 0)
    for part in range(partial.shape[0]):
        partial[part] = row[:1]
    outward.wait()


def krylov(origin, coefs, source, count, total, tables, parts):
    area, columns = source.shape
    half = columns // LANES
    rows = area - 2 * HALO
    vmem = pl.BlockSpec(memory_space=pltpu.VMEM)
    anywhere = pl.BlockSpec(memory_space=pl.ANY)
    plane = pltpu.VMEM((half, area, LANES), jnp.float32)
    padded = pltpu.VMEM((half, area + 16, LANES), jnp.float32)
    strip = pltpu.VMEM((rows, columns), jnp.float32)
    return pl.pallas_call(
        krylov_kernel,
        in_specs=[pl.BlockSpec(memory_space=pltpu.SMEM), vmem] + [anywhere] * 3 + [vmem] * 3,
        out_specs=(anywhere, vmem, vmem),
        out_shape=(
            pltpu.HBM((rows, columns), jnp.float32),
            pltpu.VMEM((ITERS, rows, columns), jnp.float32),
            pltpu.VMEM((parts, 1, LANES), jnp.float32),
        ),
        scratch_shapes=[
            pltpu.VMEM((coefs.shape[0] + 16, LANES), jnp.float32),
            pltpu.VMEM((half, area, 2 * LANES), jnp.float32),
            padded,
            plane,
            plane,
            plane,
            plane,
            plane,
            pltpu.VMEM((2, half, area + 16, LANES), jnp.float32),
            pltpu.VMEM((area, columns), jnp.float32),
            strip,
            strip,
            strip,
            pltpu.SemaphoreType.DMA((3,)),
            pltpu.SemaphoreType.DMA(()),
        ],
        compiler_params=pltpu.CompilerParams(vmem_limit_bytes=32 << 20),
        name="krylov",
    )(origin, near(coefs), far(source), far(count), far(total), *tables)


def final_kernel(partial, basis, values, pressure, loglik):
    parts = partial.shape[0]
    high = jnp.concatenate([partial[k] for k in range(parts)], axis=0)
    low = pltpu.roll(high, LANES // 2, 1)
    while high.shape[0] > 8:
        middle = high.shape[0] // 2
        top, error = two_sum(high[:middle], high[middle:])
        low = (low[:middle] + low[middle:]) + error
        high = top
    for shift in (4, 2, 1):
        high, low = fold(high, low, shift, 0)

    def pick(k):
        return (
            jnp.broadcast_to(high[:, k : k + 1], (8, LANES)),
            jnp.broadcast_to(low[:, k : k + 1], (8, LANES)),
        )

    moments = [pick(k) for k in range(TERMS)]
    matrix = [[moments[i + j + 1] for j in range(ITERS)] for i in range(ITERS)]
    right = [moments[i] for i in range(ITERS)]
    for i in range(ITERS):
        for r in range(i + 1, ITERS):
            ratio = dd_neg(dd_div(matrix[i][r], matrix[i][i]))
            for c in range(r, ITERS):
                matrix[r][c] = dd_add(matrix[r][c], dd_mul(ratio, matrix[i][c]))
            right[r] = dd_add(right[r], dd_mul(ratio, right[i]))
    weights = [None] * ITERS
    for i in reversed(range(ITERS)):
        value = right[i]
        for c in range(i + 1, ITERS):
            value = dd_add(value, dd_neg(dd_mul(matrix[i][c], weights[c])))
        weights[i] = dd_div(value, matrix[i][i])

    data = values[...]
    h, e = two_prod(data, data)
    while h.shape[0] > 8:
        middle = h.shape[0] // 2
        top, error = two_sum(h[:middle], h[middle:])
        e = (e[:middle] + e[middle:]) + error
        h = top
    for shift in (4, 2, 1):
        h, e = fold(h, e, shift, 0)
    for shift in (64, 32, 16, 8, 4, 2, 1):
        h, e = fold(h, e, shift, 1)
    misfit = (h, e)
    for spot, (i, j) in enumerate(PAIRS):
        term = dd_mul(dd_mul(weights[i], weights[j]), pick(TERMS + spot))
        misfit = dd_add(misfit, term)
        if i != j:
            misfit = dd_add(misfit, term)
    for k in range(ITERS):
        term = dd_neg(dd_mul(weights[k], pick(TERMS + len(PAIRS) + k)))
        misfit = dd_add(misfit, dd_add(term, term))
    number = values.shape[0] * LANES
    loglik[...] = (-(2.0 / number) * (misfit[0] + misfit[1]))[:1, :]

    factors = [w[0][:1, :1] for w in weights]
    for group in range(pressure.shape[0] // 8):
        put = slice(8 * group, 8 * group + 8)
        value = factors[0] * basis[0, put, :]
        for k in range(1, ITERS):
            value = value + factors[k] * basis[k, put, :]
        pressure[put, :] = value


def finish(partial, basis, values):
    vmem = pl.BlockSpec(memory_space=pltpu.VMEM)
    return pl.pallas_call(
        final_kernel,
        in_specs=[vmem] * 3,
        out_specs=(vmem, vmem),
        out_shape=(
            jax.ShapeDtypeStruct(basis.shape[1:], jnp.float32),
            jax.ShapeDtypeStruct((1, LANES), jnp.float32),
        ),
        compiler_params=pltpu.CompilerParams(vmem_limit_bytes=16 << 20),
        name="finish",
    )(near(partial), near(basis), near(values))


def exchange(block):
    return lax.all_to_all(block, "strip", split_axis=0, concat_axis=0, tiled=True)


def body(state, noise, step, field_scale, wave_scale, source, obs_cells, obs_values):
    parts = lax.axis_size("strip")
    position = lax.axis_index("strip")
    rows_here, length = state.shape
    factor = length // LANES
    half = factor // 2
    width = length // parts
    ways = parts // factor
    field_rows, columns = source.shape

    forward, inverse, special_f, special_i = dft_tables()
    cos, sin = twiddle_table(length, factor)
    across = np.float32(np.concatenate([cos, sin], 0))
    down = np.zeros((LANES, LANES), np.float32)
    down[:, :factor] = across.T

    ahead = [(i, i + 1) for i in range(parts - 1)]
    behind = [(b, a) for a, b in ahead]
    above = lax.ppermute(source[field_rows - HALO :], "strip", ahead)
    below = lax.ppermute(source[:HALO], "strip", behind)
    wide_source = jnp.concatenate([above, source, below], axis=0)

    cell_row = obs_cells // columns - position * field_rows
    count, total = observe(
        cell_row[None, :], (obs_cells % columns)[None, :], obs_values[None, :], field_rows, columns
    )

    tiles = row_forward(state, noise, step, (across, pieces(forward), pieces(special_f)))
    if ways > 1:
        tiles = tiles.reshape(factor, rows_here, ways, width).transpose(0, 2, 1, 3)
        tiles = tiles.reshape(parts, rows_here, width)
    column = exchange(tiles).reshape(factor, LANES, width)

    slot = position * width + lax.broadcasted_iota(jnp.int32, (1, width), 1)
    tile, lane = slot // LANES, slot % LANES
    middle = LANES // 2
    freq = jnp.where(
        tile == 0,
        factor * jnp.where(lane > middle, lane - middle, lane),
        jnp.where(
            tile == 1,
            half + factor * jnp.where(lane >= middle, lane - middle, lane),
            tile // 2 + factor * lane,
        ),
    )
    freq = jnp.minimum(freq, length - freq).astype(jnp.float32)
    wave = wave_scale[0]
    gain = field_scale[0] * wave / (math.sqrt(math.pi) * length)
    scale = jnp.stack([gain, wave * wave])
    blocks = column_filter(
        column,
        scale,
        freq * freq,
        (down, *(pieces(t.T) for t in (forward, special_f, inverse, special_i))),
        parts,
        field_rows,
    )
    extent = field_rows + ABOVE + BELOW
    coefs = exchange(blocks.reshape(parts, 1, extent * width))
    if ways > 1:
        coefs = coefs.reshape(factor, ways, extent, width).transpose(0, 2, 1, 3)
    coefs = coefs.reshape(factor * extent, LANES)

    origin = jnp.stack([position * field_rows, parts * field_rows]).astype(jnp.int32)
    log_perm, basis, partial = krylov(
        origin, coefs, wide_source, count, total, (across, pieces(inverse), pieces(special_i)), parts
    )
    pressure, loglik = finish(exchange(partial), basis, obs_values.reshape(-1, LANES))
    return (log_perm, pressure, loglik[0, 0])


def solution(mesh):
    placed = (P("strip", None), P("strip", None), P(), P(), P(), P("strip", None), P(), P())
    return jax.shard_map(
        body,
        mesh=mesh,
        in_specs=placed,
        out_specs=(P("strip", None), P("strip", None), P()),
        check_vma=False,
    )
```

```python
import functools
import math

import jax
import jax.numpy as jnp
import numpy as np
from jax import lax
from jax.experimental import pallas as pl
from jax.experimental.pallas import tpu as pltpu
from jax.sharding import PartitionSpec as P


ITERS = 4
LANES = 128
HALO = 8
ABOVE = ITERS
BELOW = ITERS + 1
TERMS = 2 * ITERS
PAIRS = [(i, j) for i in range(ITERS) for j in range(i, ITERS)]
SUMS = TERMS + len(PAIRS) + ITERS


def dot(left, right):
    return lax.dot_general(
        left, right, (((1,), (0,)), ((), ())), preferred_element_type=jnp.float32
    )


def halves(value):
    high = value.astype(jnp.bfloat16)
    return high, (value - high.astype(jnp.float32)).astype(jnp.bfloat16)


def rows_times(value, table):
    size = value.shape[1]
    high, low = halves(value)
    upper = table[:size, :]
    return dot(high, table[size:, :]) + dot(low, upper) + dot(high, upper)


def times_columns(table, value):
    size = value.shape[0]
    high, low = halves(value)
    upper = table[:size, :]
    return dot(table[size:, :], high) + dot(upper, low) + dot(upper, high)


def pieces(table):
    table = np.asarray(table, np.float64)
    high = table.astype(jnp.bfloat16)
    low = (table - high.astype(np.float64)).astype(jnp.bfloat16)
    return np.concatenate([high, low], 0)


def near(value):
    return pltpu.with_memory_space_constraint(value, pltpu.VMEM)


def far(value):
    return pltpu.with_memory_space_constraint(value, pltpu.HBM)


def dft_tables():
    spot = np.arange(LANES)
    angle = 2.0 * np.pi * np.outer(spot, spot) / LANES
    cos, sin = np.cos(angle), np.sin(angle)
    forward = np.block([[cos, -sin], [sin, cos]])
    inverse = np.block([[cos, sin], [-sin, cos]])
    half = LANES // 2
    whole = 2.0 * np.pi * np.outer(spot, np.arange(1, half)) / LANES
    edge = np.ones((LANES, 1))
    alternate = ((-1.0) ** spot)[:, None]
    zero_f = np.concatenate([edge, np.cos(whole), alternate, -np.sin(whole)], 1)
    zero_i = np.concatenate([edge, 2 * np.cos(whole), alternate, -2 * np.sin(whole)], 1).T
    odd = 2.0 * np.pi * np.outer(spot, np.arange(half) + 0.5) / LANES
    half_f = np.concatenate([np.cos(odd), -np.sin(odd)], 1)
    half_i = 2.0 * np.concatenate([np.cos(odd), -np.sin(odd)], 1).T
    none = np.zeros((LANES, LANES))
    special_f = np.block([[zero_f, none], [none, half_f]])
    special_i = np.block([[zero_i, none], [none, half_i]])
    return forward, inverse, special_f, special_i


def twiddle_table(length, factor):
    angle = 2.0 * np.pi * np.outer(np.arange(factor // 2), np.arange(LANES)) / length
    return np.cos(angle), np.sin(angle)


def times(value, factor):
    if value is None or factor == 0.0:
        return None
    if factor == 1.0:
        return value
    if factor == -1.0:
        return -value
    return value * factor


def plus(left, right):
    if left is None:
        return right
    if right is None:
        return left
    return left + right


def minus(left, right):
    if right is None:
        return left
    if left is None:
        return -right
    return left - right


def root(k, n):
    quarter = (8 * k) % (8 * n)
    if quarter % n == 0 and (quarter // n) % 2 == 0:
        return ((1.0, 0.0), (0.0, 1.0), (-1.0, 0.0), (0.0, -1.0))[(quarter // n) // 2]
    return (math.cos(2 * math.pi * k / n), math.sin(2 * math.pi * k / n))


def rotate(re, im, c, s):
    return (
        minus(times(re, c), times(im, s)),
        plus(times(re, s), times(im, c)),
    )


def rfft(values):
    n = len(values)
    if n == 2:
        return [(values[0] + values[1], None), (values[0] - values[1], None)]
    even = rfft(values[0::2])
    odd = rfft(values[1::2])
    out = [None] * (n // 2 + 1)
    for k in range(n // 4 + 1):
        c, s = root(k, n)
        tr, ti = rotate(odd[k][0], odd[k][1], c, -s)
        er, ei = even[k]
        out[k] = (plus(er, tr), plus(ei, ti))
        if k != n // 4:
            out[n // 2 - k] = (minus(er, tr), minus(ti, ei))
    return out


def irfft(spectrum, n):
    if n == 2:
        return [spectrum[0][0] + spectrum[1][0]]
    even, odd = [], []
    for k in range(n // 4 + 1):
        ar, ai = spectrum[k]
        br, bi = spectrum[n // 2 - k]
        if k == n // 4:
            even.append((2.0 * ar, None))
            odd.append((-2.0 * ai, None))
            continue
        even.append((plus(ar, br), minus(ai, bi)))
        c, s = root(k, n)
        odd.append(rotate(minus(ar, br), plus(ai, bi), c, s))
    even = irfft(even, n // 2)
    odd = irfft(odd, n // 2)
    return [value for pair in zip(even, odd) for value in pair]


def row_kernel(step, state, noise, twiddle, pair_w, special_w, out, work, *, factor):
    rows = state.shape[0]
    half = factor // 2
    rate = step[0]
    keep = jnp.sqrt(jnp.full((8, LANES), 1.0 - rate * rate, jnp.float32))

    def group(index, carry):
        base = pl.multiple_of(index * 8, 8)
        tiles = [
            keep * state[pl.ds(base, 8), LANES * a : LANES * (a + 1)]
            + rate * noise[pl.ds(base, 8), LANES * a : LANES * (a + 1)]
            for a in range(factor)
        ]
        spectrum = rfft(tiles)
        work[0, pl.ds(base, 8), :LANES] = spectrum[0][0]
        work[0, pl.ds(base, 8), LANES:] = spectrum[half][0]
        for j in range(1, half):
            c = twiddle[j : j + 1, :]
            s = twiddle[half + j : half + j + 1, :]
            re, im = spectrum[j]
            work[j, pl.ds(base, 8), :LANES] = re * c + im * s
            work[j, pl.ds(base, 8), LANES:] = im * c - re * s
        return carry

    lax.fori_loop(0, rows // 8, group, 0, unroll=4)
    put = slice(None)
    first = rows_times(work[0], special_w)
    out[0, put, :] = first[:, :LANES]
    out[1, put, :] = first[:, LANES:]
    batch = 5
    for begin in range(1, half, batch):
        value = rows_times(work[begin : begin + batch].reshape(batch * rows, 2 * LANES), pair_w)
        for k in range(batch):
            out[2 * (begin + k), put, :] = value[k * rows : (k + 1) * rows, :LANES]
            out[2 * (begin + k) + 1, put, :] = value[k * rows : (k + 1) * rows, LANES:]


def row_forward(state, noise, step, tables):
    rows, length = state.shape
    factor = length // LANES
    block = min(64, rows)
    twiddle, pair_w, special_w = tables
    whole = lambda i: (0, 0)
    return pl.pallas_call(
        functools.partial(row_kernel, factor=factor),
        grid=(rows // block,),
        in_specs=[
            pl.BlockSpec(memory_space=pltpu.SMEM),
            pl.BlockSpec((block, length), lambda i: (i, 0)),
            pl.BlockSpec((block, length), lambda i: (i, 0)),
            pl.BlockSpec(twiddle.shape, whole),
            pl.BlockSpec(pair_w.shape, whole),
            pl.BlockSpec(special_w.shape, whole),
        ],
        out_specs=pl.BlockSpec((factor, block, LANES), lambda i: (0, i, 0)),
        out_shape=pltpu.HBM((factor, rows, LANES), jnp.float32),
        scratch_shapes=[pltpu.VMEM((factor // 2, block, 2 * LANES), jnp.float32)],
        compiler_params=pltpu.CompilerParams(vmem_limit_bytes=16 << 20),
        name="row_forward",
    )(step, far(state), far(noise), far(twiddle), far(pair_w), far(special_w))


def column_kernel(
    origin, scale, column, table, forward_w, special_f, inverse_w, special_i, wave, count, total,
    out, work, field, *, field_rows,
):
    factor, _, width = column.shape
    half = factor // 2
    length = factor * LANES
    extent = field_rows + ABOVE + BELOW

    def ahead(index, carry):
        base = pl.multiple_of(index * 8, 8)
        spectrum = rfft([column[a, pl.ds(base, 8), :] for a in range(factor)])
        low = pl.ds(base, 8)
        high = pl.ds(pl.multiple_of(base + LANES, 8), 8)
        work[0, low, :] = spectrum[0][0]
        work[0, high, :] = spectrum[half][0]
        turn = table[low, :]
        for j in range(1, half):
            c = turn[:, j : j + 1]
            s = turn[:, half + j : half + j + 1]
            re, im = spectrum[j]
            work[j, low, :] = re * c + im * s
            work[j, high, :] = im * c - re * s
        return carry

    lax.fori_loop(0, LANES // 8, ahead, 0, unroll=4)
    place = lax.broadcasted_iota(jnp.int32, (LANES, width), 0)
    side = wave[...] + scale[1]
    gain = scale[0]

    def amplitude(freq):
        freq = jnp.minimum(freq, length - freq).astype(jnp.float32)
        return gain / (freq * freq + side)

    batch = 2 if width % LANES == 0 else 1
    for j in range(half):
        if j == 0:
            value = times_columns(special_f, work[0])
            middle = LANES // 2
            top = amplitude(factor * jnp.where(place > middle, place - middle, place))
            low = amplitude(half + factor * jnp.where(place >= middle, place - middle, place))
            value = jnp.concatenate([value[:LANES] * top, value[LANES:] * low], axis=0)
            work[0] = times_columns(special_i, value)
            continue
        if (j - 1) % batch:
            continue
        block = range(j, min(j + batch, half))
        value = times_columns(forward_w, jnp.concatenate([work[k] for k in block], axis=1))
        top = jnp.concatenate([amplitude(k + factor * place) for k in block], axis=1)
        value = jnp.concatenate([value[:LANES] * top, value[LANES:] * top], axis=0)
        value = times_columns(inverse_w, value)
        for k in block:
            work[k] = value[:, (k - j) * width : (k - j + 1) * width]

    rim = jnp.zeros((HALO, width), jnp.float32)
    field[:HALO, :] = rim
    field[HALO + length // 2 :, :] = rim

    def back(index, carry):
        base = pl.multiple_of(index * 8, 8)
        low = pl.ds(base, 8)
        high = pl.ds(pl.multiple_of(base + LANES, 8), 8)
        turn = table[low, :]
        spectrum = [(work[0, low, :], None)]
        for j in range(1, half):
            c = turn[:, j : j + 1]
            s = turn[:, half + j : half + j + 1]
            re, im = work[j, low, :], work[j, high, :]
            spectrum.append((re * c - im * s, re * s + im * c))
        spectrum.append((work[0, high, :], None))
        values = irfft(spectrum, factor)
        for a in range(half):
            field[pl.ds(pl.multiple_of(base + HALO + LANES * a, 8), 8), :] = values[a]
        return carry

    lax.fori_loop(0, LANES // 8, back, 0, unroll=4)
    for part in range(out.shape[0] // extent):
        begin = HALO - ABOVE + field_rows * part
        out[extent * part : extent * (part + 1), :] = field[begin : begin + extent, :]


def column_filter(column, scale, wave, tables, parts, field_rows, ready):
    factor, _, width = column.shape
    length = factor * LANES
    vmem = pl.BlockSpec(memory_space=pltpu.VMEM)
    return pl.pallas_call(
        functools.partial(column_kernel, field_rows=field_rows),
        in_specs=[pl.BlockSpec(memory_space=pltpu.SMEM)] * 2
        + [vmem] * 7
        + [pl.BlockSpec(memory_space=pl.ANY)] * 2,
        out_specs=vmem,
        out_shape=pltpu.VMEM((parts * (field_rows + ABOVE + BELOW), width), jnp.float32),
        scratch_shapes=[
            pltpu.VMEM((factor // 2, 2 * LANES, width), jnp.float32),
            pltpu.VMEM((length // 2 + 2 * HALO, width), jnp.float32),
        ],
        compiler_params=pltpu.CompilerParams(vmem_limit_bytes=24 << 20),
        name="column_filter",
    )(ready[0], scale, near(column), *tables, wave, *(far(value) for value in ready[1:]))


def observe_kernel(local, cells, values, count, total, left):
    rows, columns = count.shape
    block = columns
    origin = pl.program_id(0) * block

    @pl.when(pl.program_id(0) == 0)
    def _():
        row = lax.broadcasted_iota(jnp.int32, (rows, local.shape[1]), 0)
        here = row == local[...]
        value = jnp.broadcast_to(values[...], here.shape)
        first = value.astype(jnp.bfloat16).astype(jnp.float32)
        second = (value - first).astype(jnp.bfloat16).astype(jnp.float32)
        third = value - first - second
        for slot, piece in enumerate((1.0, first, second, third)):
            left[slot * rows : (slot + 1) * rows, :] = jnp.where(here, piece, 0.0).astype(jnp.bfloat16)

    spot = lax.broadcasted_iota(jnp.int32, (block, local.shape[1]), 0) + origin
    right = jnp.where(spot == cells[...], 1.0, 0.0).astype(jnp.bfloat16)
    result = lax.dot_general(
        left[...], right, (((1,), (1,)), ((), ())), preferred_element_type=jnp.float32
    )
    count[...] = result[:rows]
    total[...] = (result[3 * rows :] + result[2 * rows : 3 * rows]) + result[rows : 2 * rows]


def observe(local_row, cell_col, values, rows, columns):
    number = values.shape[1]
    block = 256
    whole = pl.BlockSpec((1, number), lambda i: (0, 0))
    piece = pl.BlockSpec((rows, block), lambda i: (0, i))
    shape = jax.ShapeDtypeStruct((rows, columns), jnp.float32)
    return pl.pallas_call(
        observe_kernel,
        compiler_params=pltpu.CompilerParams(vmem_limit_bytes=32 << 20),
        grid=(columns // block,),
        in_specs=[whole, whole, whole],
        out_specs=(piece, piece),
        out_shape=(shape, shape),
        scratch_shapes=[pltpu.VMEM((4 * rows, number), jnp.bfloat16)],
        cost_estimate=pl.CostEstimate(
            flops=8 * rows * number * columns, transcendentals=0, bytes_accessed=8 * rows * columns
        ),
        name="observe",
    )(local_row, cell_col, values)


def two_sum(a, b):
    s = a + b
    t = s - a
    return s, (a - (s - t)) + (b - t)


def split(a):
    t = a * 4097.0
    high = t - (t - a)
    return high, a - high


def two_prod(a, b):
    p = a * b
    ah, al = split(a)
    bh, bl = split(b)
    return p, ((ah * bh - p) + ah * bl + al * bh) + al * bl


def dd_add(x, y):
    s, e = two_sum(x[0], y[0])
    e = e + (x[1] + y[1])
    high = s + e
    return high, e - (high - s)


def dd_neg(x):
    return -x[0], -x[1]


def dd_mul(x, y):
    p, e = two_prod(x[0], y[0])
    e = e + (x[0] * y[1] + x[1] * y[0])
    high = p + e
    return high, e - (high - p)


def dd_div(x, y):
    first = x[0] / y[0]
    rest = dd_add(x, dd_neg(dd_mul(y, (first, jnp.zeros_like(first)))))
    second = rest[0] / y[0]
    rest = dd_add(rest, dd_neg(dd_mul(y, (second, jnp.zeros_like(first)))))
    third = rest[0] / y[0]
    high, low = two_sum(first, second)
    return dd_add((high, low), (third, jnp.zeros_like(third)))


def fold(high, low, shift, axis):
    other, error = two_sum(high, pltpu.roll(high, shift, axis))
    return other, (low + pltpu.roll(low, shift, axis)) + error


def fold_rows(value):
    pieces = [value[8 * i : 8 * i + 8] for i in range(value.shape[0] // 8)]
    while len(pieces) > 1:
        last = [pieces[-1]] if len(pieces) % 2 else []
        pieces = [a + b for a, b in zip(pieces[0::2], pieces[1::2])] + last
    return pieces[0]


def krylov_kernel(
    origin, coefs, above, middle, below, count_hbm, total_hbm, twiddle, inverse_w, special_i,
    log_perm_hbm, basis, partial,
    received, work, kappa, inverse, north, south, west, east, vector,
    source, count, total, log_perm, arrive, leave,
):
    inward = [
        pltpu.make_async_copy(far_ref, near_ref, arrive.at[k])
        for k, (far_ref, near_ref) in enumerate(
            (
                (above, source.at[:HALO, :]),
                (middle, source.at[HALO : HALO + middle.shape[0], :]),
                (below, source.at[HALO + middle.shape[0] :, :]),
                (count_hbm, count),
                (total_hbm, total),
            )
        )
    ]
    outward = pltpu.make_async_copy(log_perm, log_perm_hbm, leave)
    for copy in inward:
        copy.start()
    half, area, _ = work.shape
    factor = 2 * half
    rows = area - 2 * HALO
    extent = rows + ABOVE + BELOW
    groups = area // 8

    size = coefs.shape[0]
    rim = jnp.zeros((8, LANES), jnp.float32)
    received[:8, :] = rim
    received[8 + size : 16 + size, :] = rim
    received[8 : 8 + size, :] = coefs[...]

    def window(tile):
        begin = 8 + extent * tile + ABOVE - HALO
        return received[begin : begin + area, :]

    def pair(j):
        return jnp.concatenate([window(2 * j), window(2 * j + 1)], axis=1)

    work[0] = rows_times(pair(0), special_i)
    batch = 3
    for j in range(1, half, batch):
        value = rows_times(jnp.concatenate([pair(k) for k in range(j, j + batch)], axis=0), inverse_w)
        for k in range(batch):
            work[j + k] = value[k * area : (k + 1) * area]

    for tile in range(half):
        for ref in (kappa, vector.at[0], vector.at[1]):
            ref[tile, :8, :] = rim
            ref[tile, 8 + area :, :] = rim

    first_row = origin[0] - HALO
    limit = origin[1]

    def usable(start, count):
        local = lax.broadcasted_iota(jnp.int32, (count, LANES), 0) + start
        row = local + first_row
        inner = (local >= HALO - ABOVE) & (local < HALO + rows + BELOW)
        return inner & (row >= 0) & (row < limit)

    def inverse_group(index, carry):
        base = pl.multiple_of(index * 8, 8)
        low = pl.ds(base, 8)
        spectrum = [(work[0, low, :LANES], None)]
        for j in range(1, half):
            c = twiddle[j : j + 1, :]
            s = twiddle[half + j : half + j + 1, :]
            re, im = work[j, low, :LANES], work[j, low, LANES:]
            spectrum.append((re * c - im * s, re * s + im * c))
        spectrum.append((work[0, low, LANES:], None))
        values = irfft(spectrum, factor)
        valid = usable(base, 8)
        store = pl.ds(pl.multiple_of(base + 8, 8), 8)
        for a in range(half):
            kappa[a, store, :] = jnp.where(valid, 0.5 * jnp.exp(values[a]), 0.0)

        @pl.when((index >= HALO // 8) & (index < groups - HALO // 8))
        def _():
            own = pl.ds(pl.multiple_of(base - HALO, 8), 8)
            for a in range(half):
                log_perm[own, LANES * a : LANES * (a + 1)] = values[a]

        return carry

    lax.fori_loop(0, groups, inverse_group, 0, unroll=2)
    outward.start()
    for copy in inward[:3]:
        copy.wait()

    first_lane = lax.broadcasted_iota(jnp.int32, (1, LANES), 1) == 0
    last_lane = lax.broadcasted_iota(jnp.int32, (1, LANES), 1) == LANES - 1
    sums = [rim] * SUMS
    own = slice(HALO, HALO + rows)
    every = slice(8, 8 + area)
    before = slice(7, 7 + area)
    after = slice(9, 9 + area)

    def sideways(load):
        back, ahead = None, None
        value = load(0)
        for tile in range(half):
            following = load(tile + 1) if tile + 1 < half else None
            turned = pltpu.roll(value, 1, 1)
            ahead = pltpu.roll(value, LANES - 1, 1) if tile == 0 else ahead
            left = jnp.where(first_lane, 0.0 if back is None else back, turned)
            if following is None:
                right = jnp.where(last_lane, 0.0, ahead)
            else:
                next_ahead = pltpu.roll(following, LANES - 1, 1)
                right = jnp.where(last_lane, next_ahead, ahead)
                ahead = next_ahead
            yield tile, value, left, right
            back, value = turned, following

    valid = usable(0, area)
    for tile, here, left, right in sideways(lambda t: kappa[t, every, :]):
        lanes = slice(LANES * tile, LANES * (tile + 1))
        up = here + kappa[tile, before, :]
        down = here + kappa[tile, after, :]
        left = here + left
        right = here + right
        rest = jnp.where(valid, 1.0 / (up + down + left + right), 0.0)
        inverse[tile] = rest
        north[tile] = up
        south[tile] = down
        west[tile] = left
        east[tile] = right
        first = source[:, lanes]
        value = first * rest
        vector[0, tile, every, :] = value
        basis[0, :, lanes] = value[own]
        sums[0] = sums[0] + fold_rows((first * value)[own])

    for step in range(ITERS - 1):
        now = vector.at[step % 2]
        new = vector.at[(step + 1) % 2]
        for tile, here, left, right in sideways(lambda t: now[t, every, :]):
            image = (
                north[tile] * (here - now[tile, before, :])
                + south[tile] * (here - now[tile, after, :])
                + west[tile] * (here - left)
                + east[tile] * (here - right)
            )
            value = image * inverse[tile]
            new[tile, every, :] = value
            basis[step + 1, :, LANES * tile : LANES * (tile + 1)] = value[own]
            sums[2 * step + 1] = sums[2 * step + 1] + fold_rows((here * image)[own])
            sums[2 * step + 2] = sums[2 * step + 2] + fold_rows((value * image)[own])

    inward[3].wait()
    inward[4].wait()
    now = vector.at[(ITERS - 1) % 2]
    first = lax.broadcasted_iota(jnp.int32, (8, LANES), 0) + origin[0] == 0
    back = None
    for tile in range(half):
        lanes = slice(LANES * tile, LANES * (tile + 1))
        here = now[tile, 8 + HALO : 8 + HALO + rows, :]
        turned = pltpu.roll(here, 1, 1)
        left = jnp.where(first_lane, 0.0 if back is None else back, turned)
        back = turned
        down = here - now[tile, 9 + HALO : 9 + HALO + rows, :]
        across = here - left
        energy = fold_rows(south[tile, own, :] * (down * down) + west[tile, own, :] * (across * across))
        top = here[:8]
        energy = energy + jnp.where(first, north[tile, HALO : HALO + 8, :] * (top * top), 0.0)
        if tile == half - 1:
            energy = energy + fold_rows(jnp.where(last_lane, east[tile, own, :] * (here * here), 0.0))
        sums[TERMS - 1] = sums[TERMS - 1] + energy
        vectors = [basis[k, :, lanes] for k in range(ITERS)]
        weight = count[:, lanes]
        weighted = [weight * v for v in vectors]
        for spot, (i, j) in enumerate(PAIRS):
            sums[TERMS + spot] = sums[TERMS + spot] + fold_rows(weighted[i] * vectors[j])
        datum = total[:, lanes]
        for k in range(ITERS):
            slot = TERMS + len(PAIRS) + k
            sums[slot] = sums[slot] + fold_rows(datum * vectors[k])

    sub = lax.broadcasted_iota(jnp.int32, (8, LANES), 0)
    spot = lax.broadcasted_iota(jnp.int32, (8, LANES), 1)
    row = rim
    for begin in range(0, SUMS, 8):
        high, low = rim, rim
        for k in range(begin, min(begin + 8, SUMS)):
            h, e = sums[k], rim
            for shift in (4, 2, 1):
                h, e = fold(h, e, shift, 0)
            high = jnp.where(sub == k - begin, h, high)
            low = jnp.where(sub == k - begin, e, low)
        for shift in (64, 32, 16, 8, 4, 2, 1):
            high, low = fold(high, low, shift, 1)
        row = row + jnp.where(spot == sub + begin, high, 0.0)
        row = row + jnp.where(spot == sub + begin + LANES // 2, low, 0.0)
    for shift in (4, 2, 1):
        row = row + pltpu.roll(row, shift, 0)
    for part in range(partial.shape[0]):
        partial[part] = row[:1]
    outward.wait()


def krylov(origin, coefs, pieces_of_source, count, total, tables, parts):
    rows, columns = count.shape
    half = columns // LANES
    area = rows + 2 * HALO
    vmem = pl.BlockSpec(memory_space=pltpu.VMEM)
    anywhere = pl.BlockSpec(memory_space=pl.ANY)
    plane = pltpu.VMEM((half, area, LANES), jnp.float32)
    padded = pltpu.VMEM((half, area + 16, LANES), jnp.float32)
    strip = pltpu.VMEM((rows, columns), jnp.float32)
    return pl.pallas_call(
        krylov_kernel,
        in_specs=[pl.BlockSpec(memory_space=pltpu.SMEM), vmem] + [anywhere] * 5 + [vmem] * 3,
        out_specs=(anywhere, vmem, vmem),
        out_shape=(
            pltpu.HBM((rows, columns), jnp.float32),
            pltpu.VMEM((ITERS, rows, columns), jnp.float32),
            pltpu.VMEM((parts, 1, LANES), jnp.float32),
        ),
        scratch_shapes=[
            pltpu.VMEM((coefs.shape[0] + 16, LANES), jnp.float32),
            pltpu.VMEM((half, area, 2 * LANES), jnp.float32),
            padded,
            plane,
            plane,
            plane,
            plane,
            plane,
            pltpu.VMEM((2, half, area + 16, LANES), jnp.float32),
            pltpu.VMEM((area, columns), jnp.float32),
            strip,
            strip,
            strip,
            pltpu.SemaphoreType.DMA((5,)),
            pltpu.SemaphoreType.DMA(()),
        ],
        compiler_params=pltpu.CompilerParams(vmem_limit_bytes=32 << 20),
        name="krylov",
    )(origin, near(coefs), *(far(v) for v in (*pieces_of_source, count, total)), *tables)


def final_kernel(partial, basis, values, pressure, loglik):
    parts = partial.shape[0]
    high = jnp.concatenate([partial[k] for k in range(parts)], axis=0)
    low = pltpu.roll(high, LANES // 2, 1)
    while high.shape[0] > 8:
        middle = high.shape[0] // 2
        top, error = two_sum(high[:middle], high[middle:])
        low = (low[:middle] + low[middle:]) + error
        high = top
    for shift in (4, 2, 1):
        high, low = fold(high, low, shift, 0)

    def pick(k):
        return (
            jnp.broadcast_to(high[:, k : k + 1], (8, LANES)),
            jnp.broadcast_to(low[:, k : k + 1], (8, LANES)),
        )

    moments = [pick(k) for k in range(TERMS)]
    matrix = [[moments[i + j + 1] for j in range(ITERS)] for i in range(ITERS)]
    right = [moments[i] for i in range(ITERS)]
    for i in range(ITERS):
        for r in range(i + 1, ITERS):
            ratio = dd_neg(dd_div(matrix[i][r], matrix[i][i]))
            for c in range(r, ITERS):
                matrix[r][c] = dd_add(matrix[r][c], dd_mul(ratio, matrix[i][c]))
            right[r] = dd_add(right[r], dd_mul(ratio, right[i]))
    weights = [None] * ITERS
    for i in reversed(range(ITERS)):
        value = right[i]
        for c in range(i + 1, ITERS):
            value = dd_add(value, dd_neg(dd_mul(matrix[i][c], weights[c])))
        weights[i] = dd_div(value, matrix[i][i])

    data = values[...]
    h, e = two_prod(data, data)
    while h.shape[0] > 8:
        middle = h.shape[0] // 2
        top, error = two_sum(h[:middle], h[middle:])
        e = (e[:middle] + e[middle:]) + error
        h = top
    for shift in (4, 2, 1):
        h, e = fold(h, e, shift, 0)
    for shift in (64, 32, 16, 8, 4, 2, 1):
        h, e = fold(h, e, shift, 1)
    misfit = (h, e)
    for spot, (i, j) in enumerate(PAIRS):
        term = dd_mul(dd_mul(weights[i], weights[j]), pick(TERMS + spot))
        misfit = dd_add(misfit, term)
        if i != j:
            misfit = dd_add(misfit, term)
    for k in range(ITERS):
        term = dd_neg(dd_mul(weights[k], pick(TERMS + len(PAIRS) + k)))
        misfit = dd_add(misfit, dd_add(term, term))
    number = values.shape[0] * LANES
    loglik[...] = (-(2.0 / number) * (misfit[0] + misfit[1]))[:1, :]

    factors = [w[0][:1, :1] for w in weights]
    for group in range(pressure.shape[0] // 8):
        put = slice(8 * group, 8 * group + 8)
        value = factors[0] * basis[0, put, :]
        for k in range(1, ITERS):
            value = value + factors[k] * basis[k, put, :]
        pressure[put, :] = value


def finish(partial, basis, values):
    vmem = pl.BlockSpec(memory_space=pltpu.VMEM)
    return pl.pallas_call(
        final_kernel,
        in_specs=[vmem] * 3,
        out_specs=(vmem, vmem),
        out_shape=(
            jax.ShapeDtypeStruct(basis.shape[1:], jnp.float32),
            jax.ShapeDtypeStruct((1, LANES), jnp.float32),
        ),
        compiler_params=pltpu.CompilerParams(vmem_limit_bytes=16 << 20),
        name="finish",
    )(near(partial), near(basis), near(values))


def exchange(block):
    return lax.all_to_all(block, "strip", split_axis=0, concat_axis=0, tiled=True)


def steps(state, noise, step, field_scale, wave_scale, source, obs_cells, obs_values):
    parts = lax.axis_size("strip")
    position = lax.axis_index("strip")
    rows_here, length = state.shape
    factor = length // LANES
    half = factor // 2
    width = length // parts
    ways = parts // factor
    field_rows, columns = source.shape

    forward, inverse, special_f, special_i = dft_tables()
    cos, sin = twiddle_table(length, factor)
    across = np.float32(np.concatenate([cos, sin], 0))
    down = np.zeros((LANES, LANES), np.float32)
    down[:, :factor] = across.T

    ahead = [(i, i + 1) for i in range(parts - 1)]
    behind = [(b, a) for a, b in ahead]
    above = lax.ppermute(source[field_rows - HALO :], "strip", ahead)
    below = lax.ppermute(source[:HALO], "strip", behind)

    cell_row = obs_cells // columns - position * field_rows
    count, total = observe(
        cell_row[None, :], (obs_cells % columns)[None, :], obs_values[None, :], field_rows, columns
    )

    origin = jnp.stack([position * field_rows, parts * field_rows]).astype(jnp.int32)

    tiles = row_forward(state, noise, step, (across, pieces(forward), pieces(special_f)))
    if ways > 1:
        tiles = tiles.reshape(factor, rows_here, ways, width).transpose(0, 2, 1, 3)
        tiles = tiles.reshape(parts, rows_here, width)
    column = exchange(tiles).reshape(factor, LANES, width)

    slot = position * width + lax.broadcasted_iota(jnp.int32, (1, width), 1)
    tile, lane = slot // LANES, slot % LANES
    middle = LANES // 2
    freq = jnp.where(
        tile == 0,
        factor * jnp.where(lane > middle, lane - middle, lane),
        jnp.where(
            tile == 1,
            half + factor * jnp.where(lane >= middle, lane - middle, lane),
            tile // 2 + factor * lane,
        ),
    )
    freq = jnp.minimum(freq, length - freq).astype(jnp.float32)
    wave = wave_scale[0]
    gain = field_scale[0] * wave / (math.sqrt(math.pi) * length)
    scale = jnp.stack([gain, wave * wave])
    blocks = column_filter(
        column,
        scale,
        freq * freq,
        (down, *(pieces(t.T) for t in (forward, special_f, inverse, special_i))),
        parts,
        field_rows,
        (origin, count, total),
    )
    blocks, above, below = lax.optimization_barrier((blocks, above, below))
    extent = field_rows + ABOVE + BELOW
    coefs = exchange(blocks.reshape(parts, 1, extent * width))
    if ways > 1:
        coefs = coefs.reshape(factor, ways, extent, width).transpose(0, 2, 1, 3)
    coefs = coefs.reshape(factor * extent, LANES)

    log_perm, basis, partial = krylov(
        origin, coefs, (above, source, below), count, total, (across, pieces(inverse), pieces(special_i)), parts
    )
    pressure, loglik = finish(exchange(partial), basis, obs_values.reshape(-1, LANES))
    return (log_perm, pressure, loglik[0, 0])


def solution(mesh):
    placed = (P("strip", None), P("strip", None), P(), P(), P(), P("strip", None), P(), P())
    return jax.shard_map(
        steps,
        mesh=mesh,
        in_specs=placed,
        out_specs=(P("strip", None), P("strip", None), P()),
        check_vma=False,
    )
```
